32 devices in a mesh: segment: 4 (over y, x), amp: 8 (over z, core).
Axes of the slice: x: 2, y: 2, z: 4, core: 2. Of those that a mesh axis runs over, the one named last changes fastest.
Arguments:
- states: float32 [4, 2097152], P('segment', 'amp'), may hold values from -6 to 6
- gate_blocks: float32 [4, 3, 128, 128], P('segment'), may hold values from -1 to 1, as said below
- kraus_picks: int32 [4, 4, 3, 7], P('segment'), may hold values from 0 to 3
- block_targets: int32 [4, 3], replicated, may hold values from 0 to 1
Outputs:
- final_states: float32 [4, 2097152], P('segment', 'amp')
- log_weights: float32 [4, 4], P('segment')
The draws below stay inside these ranges and needn't reach their ends.
Inputs may be any that keep to these rules, and one draw needn't show every extreme that they name: Every block of gate_blocks is an orthogonal matrix, up to rounding.
All inputs are finite; a program needn't handle non-finite values.
Results may differ from the reference program's by a relative error of at most 0.0003.
Values sent between devices are 32-bit elements; how exact they have to be, the bound alone decides.
No kernel may reach another device: no remote copies, remote signals or barrier semaphores. Data moves between devices by JAX's collectives and lax.ppermute only.
A program may use at most 64 MiB of HBM per device.

```python
import jax
import jax.numpy as jnp
from jax import lax

QB = 7
REG = 128
MIDC = 16
BLOCKS = 3
SECTIONS = 4
TRAJ = 4
GLOBALS = 8
AMPS = 2097152


def draw_gate_blocks(key, part):
    gaussian = jax.random.normal(key, (SECTIONS, BLOCKS, REG, REG), jnp.float32)
    q_factor, r_factor = jnp.linalg.qr(gaussian)
    return q_factor.astype(jnp.float32)


def place_ends(array, key, low, largest):
    place = [jax.random.randint(jax.random.fold_in(key, axis), (), 0, length) for axis, length in enumerate(array.shape)]
    main_axis = array.shape.index(max(array.shape))
    beside = place[:main_axis] + [(place[main_axis] + 1) % array.shape[main_axis]] + place[main_axis + 1:]
    return array.at[tuple(place)].set(low).at[tuple(beside)].set(largest)


def level_of(rng, extent, shards, smallest, largest):
    factor_of = 1.0
    for axis_at, shards_of in shards:
        heights = jax.random.uniform(jax.random.fold_in(jax.random.fold_in(rng, 6), axis_at), (shards_of,), jnp.float32, smallest / len(shards), largest / len(shards))
        factor_of = factor_of * jnp.repeat(jnp.exp(heights), extent[axis_at] // shards_of).reshape((-1,) + (1,) * (len(extent) - 1 - axis_at))
    return factor_of


def normal_values(own_key, extent, deviation, most, cuts=(), kind=jnp.bfloat16):
    gain = level_of(own_key, extent, cuts, -0.22, 0.18) if cuts else 1.0
    values = jax.random.normal(own_key, extent, jnp.float32) * deviation * gain
    return jnp.minimum(jnp.maximum(values, -most), most).astype(kind)


def setup_inputs(seed: int = 0) -> dict:
    arg_keys = jax.random.split(jax.random.key(seed), 5)
    states = normal_values(arg_keys[0], (TRAJ, AMPS), 1.0, 6.0, ((0, 4), (1, 8)), jnp.float32)
    gate_blocks = draw_gate_blocks(jax.random.fold_in(arg_keys[4], 71), 0)
    kraus_picks = place_ends(jax.random.randint(arg_keys[2], (TRAJ, SECTIONS, BLOCKS, QB), 0, 4), jax.random.fold_in(arg_keys[2], 1), 0, 3).astype(jnp.int32)
    block_targets = place_ends(jax.random.randint(arg_keys[3], (SECTIONS, BLOCKS), 0, 2), jax.random.fold_in(arg_keys[3], 1), 0, 1).astype(jnp.int32)
    return {"states": states, "gate_blocks": gate_blocks, "kraus_picks": kraus_picks, "block_targets": block_targets}


KEEP_FACTORS = (1.0, 0.9, 1.0, 0.97)
FLIP_FACTORS = (0.9, 1.0, 0.97, 1.0)

def noise_factors(kraus_rows):
    qubit_count = kraus_rows.shape[-1]
    register = 2 ** qubit_count
    positions = jnp.arange(register, dtype=jnp.int32)
    product = jnp.ones(kraus_rows.shape[:-1] + (register,), jnp.float32)
    for qubit_pos in range(qubit_count):
        bit_value = jnp.right_shift(positions, qubit_count - 1 - qubit_pos) & 1
        column = kraus_rows[..., qubit_pos:qubit_pos + 1]
        low_value = jnp.zeros(column.shape, jnp.float32)
        high_value = jnp.zeros(column.shape, jnp.float32)
        for option in range(4):
            picked = (column == option).astype(jnp.float32)
            low_value = low_value + picked * KEEP_FACTORS[option]
            high_value = high_value + picked * FLIP_FACTORS[option]
        product = product * jnp.where(bit_value == 1, high_value, low_value)
    return product

def apply_gate(amplitudes, matrix, factors, target):

    def on_low(values):
        mixed_rows = jnp.einsum('bghmk,ik->bghmi', values, matrix, precision=lax.Precision.HIGHEST)
        return mixed_rows * factors[:, None, None, None, :]

    def on_high(values):
        mixed_rows = jnp.einsum('bgjmk,ij->bgimk', values, matrix, precision=lax.Precision.HIGHEST)
        return mixed_rows * factors[:, None, :, None, None]
    return lax.cond(target == 0, on_low, on_high, amplitudes)

def swap_global(amplitudes):
    traj_all, global_count, register, middle, low_count = amplitudes.shape
    split_view = amplitudes.reshape(traj_all, global_count, global_count, register // global_count, middle, low_count)
    swapped = jnp.swapaxes(split_view, 1, 2)
    return swapped.reshape(traj_all, global_count, register, middle, low_count)

def reference(states, gate_blocks, kraus_picks, block_targets):
    register = gate_blocks.shape[-1]
    amplitudes = states.reshape(TRAJ, GLOBALS, register, MIDC, register)
    mean_sq = lax.optimization_barrier(jnp.mean(amplitudes * amplitudes, axis=(1, 2, 3, 4)))
    amplitudes = amplitudes / jnp.sqrt(mean_sq)[:, None, None, None, None]
    log_list = []
    for section in range(SECTIONS):
        for block_pos in range(BLOCKS):
            factors = noise_factors(kraus_picks[:, section, block_pos, :])
            amplitudes = apply_gate(amplitudes, gate_blocks[section, block_pos], factors, block_targets[section, block_pos])
        amplitudes = swap_global(amplitudes)
        mean_sq = lax.optimization_barrier(jnp.mean(amplitudes * amplitudes, axis=(1, 2, 3, 4)))
        log_list.append(jnp.log(mean_sq))
        amplitudes = amplitudes / jnp.sqrt(mean_sq)[:, None, None, None, None]
    return (amplitudes.reshape(TRAJ, AMPS), jnp.stack(log_list, axis=1))
```

```python
import functools

import jax
import jax.numpy as jnp
from jax import lax
from jax.experimental import pallas as pl
from jax.experimental.pallas import tpu as pltpu
from jax.sharding import PartitionSpec as P

KEEP_FACTORS = (1.0, 0.9, 1.0, 0.97)
FLIP_FACTORS = (0.9, 1.0, 0.97, 1.0)
F32 = jnp.float32
BF16 = jnp.bfloat16
VMEM = pl.BlockSpec(memory_space=pltpu.VMEM)
SMEM = pl.BlockSpec(memory_space=pltpu.SMEM)
EXTRA = 8


def split(value):
    high = value.astype(BF16)
    return high, (value - high.astype(F32)).astype(BF16)


def mm(a, b):
    return jnp.dot(a, b, preferred_element_type=F32)


def mm3(a_high, a_low, b_high, b_low):
    return mm(a_high, b_high) + (mm(a_high, b_low) + mm(a_low, b_high))


def pack_kernel(chunks, middle, peers, x_ref, *out_refs):
    me = lax.axis_index("amp")
    register = out_refs[0].shape[0]
    for at, (chunk, k) in enumerate(peers):
        m = (me ^ k) * chunks + chunk
        out_refs[at][...] = x_ref[pl.ds(m, register, stride=middle), :]


def noise_column(picks_ref, at, qubits, register):
    rows = lax.broadcasted_iota(jnp.int32, (register, register), 0)
    product = jnp.ones((register, register), F32)
    for q in range(qubits):
        pick = picks_ref[at * qubits + q]
        low = jnp.where(pick == 0, KEEP_FACTORS[0], jnp.where(pick == 1, KEEP_FACTORS[1], jnp.where(pick == 2, KEEP_FACTORS[2], KEEP_FACTORS[3])))
        high = jnp.where(pick == 0, FLIP_FACTORS[0], jnp.where(pick == 1, FLIP_FACTORS[1], jnp.where(pick == 2, FLIP_FACTORS[2], FLIP_FACTORS[3])))
        bit = jnp.right_shift(rows, qubits - 1 - q) & 1
        product = product * jnp.where(bit == 1, high, low)
    return product


def combine_kernel(sections, blocks, qubits, picks_ref, targets_ref, *refs):
    gate_refs, (low_high, low_low, high_high, high_low) = refs[:sections], refs[sections:]
    seg = lax.axis_index("segment")
    register = gate_refs[0].shape[-1]
    rows = lax.broadcasted_iota(jnp.int32, (register, register), 0)
    columns = lax.broadcasted_iota(jnp.int32, (register, register), 1)
    eye = (rows == columns).astype(F32)
    for k in range(sections):
        section = seg ^ k
        low, high = eye, eye
        for block in range(blocks):
            on_low = targets_ref[section * blocks + block] == 0
            gate = gate_refs[k][block] * noise_column(picks_ref, section * blocks + block, qubits, register)
            if block == 0:
                moved = gate
            else:
                moved = jnp.dot(gate, jnp.where(on_low, low, high), precision=lax.Precision.HIGHEST, preferred_element_type=F32)
            low, high = jnp.where(on_low, moved, low), jnp.where(on_low, high, moved)
        low_high[section], low_low[section] = split(low.T)
        high_high[section], high_low[section] = split(high)


def sections_kernel(sections, amp, last, *refs):
    received = refs[:amp]
    low_high, low_low, high_high, high_low = refs[amp : amp + 4]
    at = amp + 4
    if last:
        sums_in, at = refs[at], at + 1
    outs, at = refs[at : at + amp], at + amp
    if not last:
        sums_out, at = refs[at], at + 1
    (x,) = refs[at:]
    me = lax.axis_index("amp")
    register, lanes = received[0].shape
    rest = register // amp

    def squares(total, value):
        return total + jnp.sum(value * value, axis=0, keepdims=True)

    sums = []
    total = jnp.zeros((1, lanes), F32)
    for k in range(amp):
        value = received[k][...]
        total = squares(total, value)
        x[me ^ k] = value
    sums.append(total)
    for section in range(sections):
        ll, lh = low_low[section], low_high[section]
        hl, hh = high_low[section], high_high[section]
        total = jnp.zeros((1, lanes), F32)
        for part in range(amp):
            if section % 2 == 0:
                value = x[part]
            else:
                value = x[:, part * rest : (part + 1) * rest, :].reshape(register, lanes)
            value = mm3(*split(value), lh, ll)
            value = mm3(hh, hl, *split(value))
            total = squares(total, value)
            if section % 2 == 0:
                x[part] = value
            else:
                x[:, part * rest : (part + 1) * rest, :] = value.reshape(amp, rest, lanes)
        sums.append(total)
    rows = jnp.concatenate(sums + [jnp.zeros((EXTRA - len(sums), lanes), F32)], axis=0)
    if last:
        rows = rows + sums_in[...]
    else:
        sums_out[...] = rows
    for k in range(amp):
        outs[k][0:register, :] = x[me ^ k]
        if last:
            outs[k][register:, :] = rows


def unpack_kernel(chunks, amp, middle, sections, total_amps, *refs):
    pieces, (x_ref, logs_ref) = refs[: chunks * amp], refs[chunks * amp :]
    me = lax.axis_index("amp")
    register, lanes = pieces[0].shape
    totals = pieces[(chunks - 1) * amp][register:, :]
    for k in range(1, amp):
        totals = totals + pieces[(chunks - 1) * amp + k][register:, :]
    totals = jnp.sum(totals, axis=1, keepdims=True)
    logs = jnp.log(totals[1 : sections + 1] / totals[:sections])
    spread = lax.broadcasted_iota(jnp.int32, (sections, sections), 0) == lax.broadcasted_iota(jnp.int32, (sections, sections), 1)
    logs_ref[...] = jnp.sum(jnp.where(spread, logs, 0.0), axis=0, keepdims=True)
    scale = 1.0 / jnp.sqrt(totals[sections : sections + 1] / total_amps)
    for chunk in range(chunks):
        for k in range(amp):
            m = (me ^ k) * chunks + chunk
            x_ref[pl.ds(m, register, stride=middle), :] = pieces[chunk * amp + k][0:register, :] * scale


def exchange(piece, k, size, axis):
    if k == 0:
        return piece
    return lax.ppermute(piece, axis, [(i, i ^ k) for i in range(size)])


def body_fast(states, gate_blocks, kraus_picks, block_targets):
    amp_local = states.shape[1]
    register = gate_blocks.shape[-1]
    blocks = gate_blocks.shape[1]
    qubits = kraus_picks.shape[-1]
    amp, sections = lax.axis_size("amp"), lax.axis_size("segment")
    middle = amp_local // (register * register)
    chunks = middle // amp
    piece = jax.ShapeDtypeStruct((register, register), F32)
    tall = jax.ShapeDtypeStruct((register + EXTRA, register), F32)
    order = list(range(amp - 1, -1, -1))

    x = states.reshape(register * middle, register)
    peers = [(chunk, k) for chunk in range(chunks) for k in range(amp)]
    packed = pl.pallas_call(
        functools.partial(pack_kernel, chunks, middle, peers),
        out_shape=[piece] * len(peers),
        in_specs=[VMEM],
        out_specs=[VMEM] * len(peers),
        name="pack",
    )(x)
    packed = dict(zip(peers, packed))
    received = {}
    for chunk in range(chunks):
        for k in order:
            received[chunk, k] = exchange(packed[chunk, k], k, amp, "amp")

    gates = [exchange(gate_blocks[0], k, sections, "segment") for k in range(sections)]
    matrix = jax.ShapeDtypeStruct((sections, register, register), BF16)
    matrices = pl.pallas_call(
        functools.partial(combine_kernel, sections, blocks, qubits),
        out_shape=[matrix] * 4,
        in_specs=[SMEM, SMEM] + [VMEM] * sections,
        out_specs=[VMEM] * 4,
        name="combine",
    )(kraus_picks.reshape(-1), block_targets.reshape(-1), *gates)

    sums = jax.ShapeDtypeStruct((EXTRA, register), F32)
    returned = {}
    carried = []
    for chunk in range(chunks):
        last = chunk == chunks - 1
        results = pl.pallas_call(
            functools.partial(sections_kernel, sections, amp, last),
            out_shape=[tall] * amp if last else [piece] * amp + [sums],
            in_specs=[VMEM] * (amp + 4 + len(carried)),
            out_specs=[VMEM] * (amp if last else amp + 1),
            scratch_shapes=[pltpu.VMEM((amp, register, register), F32)],
            name="sections",
        )(*[received[chunk, k] for k in range(amp)], *matrices, *carried)
        carried = [] if last else [results[amp]]
        for k in order:
            returned[chunk, k] = exchange(results[k], k, amp, "amp")

    out, logs = pl.pallas_call(
        functools.partial(unpack_kernel, chunks, amp, middle, sections, float(amp_local * amp)),
        out_shape=[jax.ShapeDtypeStruct((register * middle, register), F32), jax.ShapeDtypeStruct((1, sections), F32)],
        in_specs=[VMEM] * (chunks * amp),
        out_specs=[VMEM, VMEM],
        name="unpack",
    )(*[returned[chunk, k] for chunk, k in peers])
    return out.reshape(1, amp_local), logs


def noise_factors(kraus_rows):
    qubit_count = kraus_rows.shape[-1]
    register = 2**qubit_count
    positions = jnp.arange(register, dtype=jnp.int32)
    product = jnp.ones(kraus_rows.shape[:-1] + (register,), jnp.float32)
    for qubit_pos in range(qubit_count):
        bit_value = jnp.right_shift(positions, qubit_count - 1 - qubit_pos) & 1
        column = kraus_rows[..., qubit_pos : qubit_pos + 1]
        low_value = jnp.zeros(column.shape, jnp.float32)
        high_value = jnp.zeros(column.shape, jnp.float32)
        for option in range(4):
            picked = (column == option).astype(jnp.float32)
            low_value = low_value + picked * KEEP_FACTORS[option]
            high_value = high_value + picked * FLIP_FACTORS[option]
        product = product * jnp.where(bit_value == 1, high_value, low_value)
    return product


def apply_gate(amplitudes, matrix, factors, target):

    def on_low(values):
        mixed_rows = jnp.einsum("bhmk,ik->bhmi", values, matrix, precision=lax.Precision.HIGHEST)
        return mixed_rows * factors[:, None, None, :]

    def on_high(values):
        mixed_rows = jnp.einsum("bjmk,ij->bimk", values, matrix, precision=lax.Precision.HIGHEST)
        return mixed_rows * factors[:, :, None, None]

    return lax.cond(target == 0, on_low, on_high, amplitudes)


def square_sums(values):
    return (values, jnp.sum(values * values, axis=(1, 2, 3)))


def body_general(states, gate_blocks, kraus_picks, block_targets):
    traj_here = states.shape[0]
    amp_local = states.shape[1]
    register = gate_blocks.shape[-1]
    blocks = gate_blocks.shape[1]
    middle = amp_local // (register * register)
    total_amps = amp_local * lax.axis_size("amp")
    sections = lax.axis_size("segment")
    amplitudes = states.reshape(traj_here, register, middle, register)
    local_sums = [jnp.sum(amplitudes * amplitudes, axis=(1, 2, 3))]
    for section in range(sections):
        owned = jnp.where(lax.axis_index("segment") == section, gate_blocks, jnp.zeros_like(gate_blocks))
        section_gates = lax.psum(owned, "segment")[0]
        for block_pos in range(blocks):
            factors = noise_factors(kraus_picks[:, section, block_pos, :])
            amplitudes = apply_gate(
                amplitudes, section_gates[block_pos], factors, block_targets[section, block_pos]
            )
        amplitudes, local_sq = square_sums(
            lax.all_to_all(amplitudes, "amp", split_axis=1, concat_axis=1, tiled=True)
        )
        local_sums.append(local_sq)
    totals = lax.psum(jnp.stack(local_sums, axis=1), "amp")
    log_weights = jnp.log(totals[:, 1:] / totals[:, :-1])
    amplitudes = amplitudes / jnp.sqrt(totals[:, -1] / total_amps)[:, None, None, None]
    return (amplitudes.reshape(traj_here, amp_local), log_weights)


def solution(mesh):
    in_specs = (
        P("segment", "amp"),
        P("segment", None, None, None),
        P("segment", None, None, None),
        P(),
    )
    out_specs = (P("segment", "amp"), P("segment", None))

    def body(states, gate_blocks, kraus_picks, block_targets):
        amp, sections = lax.axis_size("amp"), lax.axis_size("segment")
        register = gate_blocks.shape[-1]
        middle = states.shape[1] // (register * register)
        power_of_two = amp & (amp - 1) == 0 and sections & (sections - 1) == 0
        fits = middle % amp == 0 and register % (8 * amp) == 0
        fast = power_of_two and fits and sections % 2 == 0 and sections < EXTRA and states.shape[0] == 1
        run = body_fast if fast else body_general
        return run(states, gate_blocks, kraus_picks, block_targets)

    return jax.shard_map(body, mesh=mesh, in_specs=in_specs, out_specs=out_specs, check_vma=False)
```

```python
import functools

import jax
import jax.numpy as jnp
from jax import lax
from jax.experimental import pallas as pl
from jax.experimental.pallas import tpu as pltpu
from jax.sharding import PartitionSpec as P


KEEP_FACTORS = (1.0, 0.9, 1.0, 0.97)
FLIP_FACTORS = (0.9, 1.0, 0.97, 1.0)
F32 = jnp.float32
BF16 = jnp.bfloat16
VMEM = pl.BlockSpec(memory_space=pltpu.VMEM)
SMEM = pl.BlockSpec(memory_space=pltpu.SMEM)
EXTRA = 8
VMEM_LIMIT = 12 * 2**20


def split(value):
    high = value.astype(BF16)
    return high, (value - high.astype(F32)).astype(BF16)


def pack_kernel(x_ref, *out_refs):
    me = lax.axis_index("amp")
    register, middle, lanes = x_ref.shape
    rows = x_ref.reshape(register * middle, lanes)
    for far, out in enumerate(out_refs):
        for near in range(2):
            out[near] = rows[pl.ds(me ^ (2 * far + near), register, stride=middle), :]


def pack_both_kernel(x_ref, side_ref, *out_refs):
    me = lax.axis_index("amp")
    register, middle, lanes = x_ref.shape
    for near, ref in enumerate((x_ref, side_ref)):
        rows = ref.reshape(register * middle, lanes)
        for far, out in enumerate(out_refs):
            out[near] = rows[pl.ds(me ^ (2 * far), register, stride=middle), :]


def part_kernel(*refs):
    lines = len(refs) - 2
    for far in range(lines):
        refs[lines][far] = refs[far][0]
        refs[lines + 1][far] = refs[far][1]


def join_kernel(own_ref, other_ref, *out_refs):
    for far, out in enumerate(out_refs):
        out[0] = own_ref[far]
        out[1] = other_ref[far]


def pick_of(pick, factors):
    value = jnp.float32(factors[-1])
    for option in range(len(factors) - 1):
        value = jnp.where(pick == option, factors[option], value)
    return value


def noise_rows(picks_ref, section, block, register):
    rows = lax.broadcasted_iota(jnp.int32, (register, register), 0)
    product = jnp.ones((register, register), F32)
    qubits = picks_ref.shape[-1]
    for q in range(qubits):
        pick = picks_ref[section, block, q]
        bit = jnp.right_shift(rows, qubits - 1 - q) & 1
        product = product * jnp.where(bit == 1, pick_of(pick, FLIP_FACTORS), pick_of(pick, KEEP_FACTORS))
    return product


def combine_kernel(sections, picks_ref, targets_ref, *refs):
    gate_refs, (low_ref, high_ref) = refs[:sections], refs[sections:]
    seg = lax.axis_index("segment")
    blocks, register = gate_refs[0].shape[0], gate_refs[0].shape[-1]
    rows = lax.broadcasted_iota(jnp.int32, (register, register), 0)
    columns = lax.broadcasted_iota(jnp.int32, (register, register), 1)
    eye = (rows == columns).astype(F32)
    zero = jnp.zeros((register, register), BF16)
    for k in range(sections):
        section = seg ^ k
        low, high = eye, eye
        for block in range(blocks):
            on_low = targets_ref[section, block] == 0
            moved = gate_refs[k][block] * noise_rows(picks_ref, section, block, register)
            if block > 0:
                before = jnp.where(on_low, low, high)
                moved = jnp.dot(moved, before, precision=lax.Precision.HIGHEST, preferred_element_type=F32)
            low, high = jnp.where(on_low, moved, low), jnp.where(on_low, high, moved)
        big, small = split(low.T)
        low_ref[section] = jnp.concatenate(
            [jnp.concatenate([big, small], axis=1), jnp.concatenate([big, zero], axis=1)], axis=0
        )
        big, small = split(high)
        high_ref[section] = jnp.concatenate(
            [jnp.concatenate([big, big], axis=1), jnp.concatenate([small, zero], axis=1)], axis=0
        )


def on_low(value, weights):
    lanes = value.shape[1]
    both = jnp.dot(jnp.concatenate(split(value), axis=1), weights, preferred_element_type=F32)
    return both[:, :lanes] + both[:, lanes:]


def on_high(value, weights):
    rows = value.shape[0] // 2
    wide = jnp.concatenate([value[:rows], value[rows:]], axis=1)
    both = jnp.dot(weights, jnp.concatenate(split(wide), axis=0), preferred_element_type=F32)
    both = both[:rows] + both[rows:]
    lanes = value.shape[1]
    return jnp.concatenate([both[:, :lanes], both[:, lanes:]], axis=0)


def piece_of(refs, far, near):
    return refs[near].at[far] if len(refs) == 2 else refs[far].at[near]


def sections_kernel(sections, lines, pieces, last, *refs):
    amp = 2 * lines
    piece_refs, (low_ref, high_ref) = refs[:pieces], refs[pieces : pieces + 2]
    at = pieces + 2
    if last:
        sums_in, at = refs[at], at + 1
    out_refs, x = refs[at:-1], refs[-1]
    me = lax.axis_index("amp")
    register, lanes = piece_refs[0].shape[-2:]
    rest = register // amp

    def squares(total, value):
        return total + jnp.sum(value * value, axis=0, keepdims=True)

    total = jnp.zeros((1, lanes), F32)
    for far in range(lines):
        for near in range(2):
            value = piece_of(piece_refs, far, near)[...]
            total = squares(total, value)
            x[me ^ (2 * far + near)] = value
    sums = [total]
    for section in range(sections):
        low, high = low_ref[section], high_ref[section]
        total = jnp.zeros((1, lanes), F32)
        for pair in range(lines):
            parts = (2 * pair, 2 * pair + 1)
            if section % 2 == 0:
                value = jnp.concatenate([x[part] for part in parts], axis=0)
            else:
                spans = [x[:, part * rest : (part + 1) * rest, :].reshape(register, lanes) for part in parts]
                value = jnp.concatenate(spans, axis=0)
            value = on_high(on_low(value, low), high)
            total = squares(total, value)
            for half, part in enumerate(parts):
                piece = value[half * register : (half + 1) * register]
                if section % 2 == 0:
                    x[part] = piece
                else:
                    x[:, part * rest : (part + 1) * rest, :] = piece.reshape(amp, rest, lanes)
        sums.append(total)
    rows = jnp.concatenate(sums + [jnp.zeros((EXTRA - len(sums), lanes), F32)], axis=0)
    if last:
        rows = rows + sums_in[...]
    else:
        out_refs[lines][...] = rows
    for far in range(lines):
        for near in range(2):
            out = piece_of(out_refs if last else out_refs[:lines], far, near)
            out[0:register, :] = x[me ^ (2 * far + near)]
            if last:
                out[register:, :] = rows


def unpack_kernel(lines, counts, total_amps, *refs):
    held = []
    for count in counts:
        held, refs = held + [refs[:count]], refs[count:]
    x_ref, logs_ref = refs
    me = lax.axis_index("amp")
    register, middle, lanes = x_ref.shape
    sections = logs_ref.shape[1]
    totals = jnp.zeros((EXTRA, lanes), F32)
    for far in range(lines):
        for near in range(2):
            totals = totals + piece_of(held[-1], far, near)[register:, :]
    totals = jnp.sum(totals, axis=1, keepdims=True)
    logs = jnp.log(totals[1 : sections + 1] / totals[:sections])
    rows = lax.broadcasted_iota(jnp.int32, (sections, sections), 0)
    columns = lax.broadcasted_iota(jnp.int32, (sections, sections), 1)
    logs_ref[...] = jnp.sum(jnp.where(rows == columns, logs, 0.0), axis=0, keepdims=True)
    scale = 1.0 / jnp.sqrt(totals[sections : sections + 1] / total_amps)
    out = x_ref.reshape(register * middle, lanes)
    for chunk, pieces in enumerate(held):
        for far in range(lines):
            for near in range(2):
                value = piece_of(pieces, far, near)[0:register, :]
                m = chunk * 2 * lines + (me ^ (2 * far + near))
                out[pl.ds(m, register, stride=middle), :] = value * scale


def swap(piece, k, size, axis):
    if k == 0:
        return piece
    return lax.ppermute(piece, axis, [(i, i ^ k) for i in range(size)])


def body_fast(states, gate_blocks, kraus_picks, block_targets):
    amp_local = states.shape[1]
    register = gate_blocks.shape[-1]
    amp, sections = lax.axis_size("amp"), lax.axis_size("segment")
    middle = amp_local // (register * register)
    chunks, lines = middle // amp, amp // 2
    params = pltpu.CompilerParams(vmem_limit_bytes=VMEM_LIMIT)

    def array(*shape, dtype=F32):
        return jax.ShapeDtypeStruct(shape, dtype)

    def kernel(body, out_shape, *operands, in_specs=None, **options):
        specs = dict(in_specs=in_specs or [VMEM] * len(operands))
        if "grid" not in options:
            specs["out_specs"] = [VMEM] * len(out_shape)
        return pl.pallas_call(body, out_shape=out_shape, compiler_params=params, **specs, **options)(*operands)

    def along(pieces):
        back = {far: swap(pieces[far], 2 * far, amp, "amp") for far in range(lines - 1, -1, -1)}
        return [back[far] for far in range(lines)]

    def across(piece):
        return swap(piece, 1, amp, "amp")

    pairs, halves = [array(2, register, register)] * lines, [array(lines, register, register)] * 2
    x = states.reshape(register, middle, register)
    arrived = []
    for chunk in range(chunks):
        if chunk == 0:
            packed = kernel(
                pack_kernel,
                pairs,
                pltpu.with_memory_space_constraint(x, pltpu.HBM),
                grid=(1,),
                in_specs=[pl.BlockSpec((register, amp, register), lambda i: (0, 0, 0))],
                out_specs=[pl.BlockSpec((2, register, register), lambda i: (0, 0, 0))] * lines,
            )
            near, other = kernel(part_kernel, halves, *along(packed))
            arrived.append([near, across(other)])
        else:
            own = x[:, chunk * amp : (chunk + 1) * amp, :]
            packed = kernel(pack_both_kernel, pairs, own, across(own))
            arrived.append(along(packed))

    gates = [swap(gate_blocks[0], k, sections, "segment") for k in range(sections)]
    low, high = kernel(
        functools.partial(combine_kernel, sections),
        [array(sections, 2 * register, 2 * register, dtype=BF16)] * 2,
        kraus_picks[0],
        block_targets,
        *gates,
        in_specs=[SMEM, SMEM] + [VMEM] * sections,
    )

    carried, held = [], []
    for chunk, pieces in enumerate(arrived):
        last = chunk == chunks - 1
        results = kernel(
            functools.partial(sections_kernel, sections, lines, len(pieces), last),
            [array(lines, register + EXTRA, register)] * 2 if last else pairs + [array(EXTRA, register)],
            *pieces,
            low,
            high,
            *carried,
            scratch_shapes=[pltpu.VMEM((amp, register, register), F32)],
        )
        if last:
            own, other = results
            tall = [array(2, register + EXTRA, register)] * lines
            joined = kernel(join_kernel, tall, own, across(other))
            held.append(along(joined))
        else:
            carried = [results[lines]]
            near, other = kernel(part_kernel, halves, *along(results[:lines]))
            held.append([near, across(other)])

    out, logs = kernel(
        functools.partial(unpack_kernel, lines, [len(pieces) for pieces in held], float(amp_local * amp)),
        [array(register, middle, register), array(1, sections)],
        *[piece for pieces in held for piece in pieces],
    )
    return out.reshape(1, amp_local), logs


def noise_factors(kraus_rows):
    qubit_count = kraus_rows.shape[-1]
    register = 2**qubit_count
    positions = jnp.arange(register, dtype=jnp.int32)
    product = jnp.ones(kraus_rows.shape[:-1] + (register,), jnp.float32)
    for qubit_pos in range(qubit_count):
        bit_value = jnp.right_shift(positions, qubit_count - 1 - qubit_pos) & 1
        column = kraus_rows[..., qubit_pos : qubit_pos + 1]
        low_value = jnp.zeros(column.shape, jnp.float32)
        high_value = jnp.zeros(column.shape, jnp.float32)
        for option in range(4):
            picked = (column == option).astype(jnp.float32)
            low_value = low_value + picked * KEEP_FACTORS[option]
            high_value = high_value + picked * FLIP_FACTORS[option]
        product = product * jnp.where(bit_value == 1, high_value, low_value)
    return product


def apply_gate(amplitudes, matrix, factors, target):

    def on_low(values):
        mixed_rows = jnp.einsum("bhmk,ik->bhmi", values, matrix, precision=lax.Precision.HIGHEST)
        return mixed_rows * factors[:, None, None, :]

    def on_high(values):
        mixed_rows = jnp.einsum("bjmk,ij->bimk", values, matrix, precision=lax.Precision.HIGHEST)
        return mixed_rows * factors[:, :, None, None]

    return lax.cond(target == 0, on_low, on_high, amplitudes)


def square_sums(values):
    return (values, jnp.sum(values * values, axis=(1, 2, 3)))


def body_general(states, gate_blocks, kraus_picks, block_targets):
    traj_here = states.shape[0]
    amp_local = states.shape[1]
    register = gate_blocks.shape[-1]
    blocks = gate_blocks.shape[1]
    middle = amp_local // (register * register)
    total_amps = amp_local * lax.axis_size("amp")
    sections = lax.axis_size("segment")
    amplitudes = states.reshape(traj_here, register, middle, register)
    local_sums = [jnp.sum(amplitudes * amplitudes, axis=(1, 2, 3))]
    for section in range(sections):
        owned = jnp.where(lax.axis_index("segment") == section, gate_blocks, jnp.zeros_like(gate_blocks))
        section_gates = lax.psum(owned, "segment")[0]
        for block_pos in range(blocks):
            factors = noise_factors(kraus_picks[:, section, block_pos, :])
            amplitudes = apply_gate(
                amplitudes, section_gates[block_pos], factors, block_targets[section, block_pos]
            )
        amplitudes, local_sq = square_sums(
            lax.all_to_all(amplitudes, "amp", split_axis=1, concat_axis=1, tiled=True)
        )
        local_sums.append(local_sq)
    totals = lax.psum(jnp.stack(local_sums, axis=1), "amp")
    log_weights = jnp.log(totals[:, 1:] / totals[:, :-1])
    amplitudes = amplitudes / jnp.sqrt(totals[:, -1] / total_amps)[:, None, None, None]
    return (amplitudes.reshape(traj_here, amp_local), log_weights)


def solution(mesh):
    in_specs = (
        P("segment", "amp"),
        P("segment", None, None, None),
        P("segment", None, None, None),
        P(),
    )
    out_specs = (P("segment", "amp"), P("segment", None))
    amp, sections = mesh.shape["amp"], mesh.shape["segment"]

    def run(states, gate_blocks, kraus_picks, block_targets):
        register = gate_blocks.shape[-1]
        middle = states.shape[1] // amp // (register * register)
        power_of_two = amp > 1 and amp & (amp - 1) == 0 and sections & (sections - 1) == 0
        fits = middle > 0 and middle % amp == 0 and register % (8 * amp) == 0
        fast = power_of_two and fits and sections % 2 == 0 and sections < EXTRA and states.shape[0] == sections

        def body(*args):
            return (body_fast if fast else body_general)(*args)

        step = jax.shard_map(body, mesh=mesh, in_specs=in_specs, out_specs=out_specs, check_vma=False)
        return step(states, gate_blocks, kraus_picks, block_targets)

    return run
```

```python
import functools

import jax
import jax.numpy as jnp
from jax import lax
from jax.experimental import pallas as pl
from jax.experimental.pallas import tpu as pltpu
from jax.sharding import PartitionSpec as P


KEEP_FACTORS = (1.0, 0.9, 1.0, 0.97)
FLIP_FACTORS = (0.9, 1.0, 0.97, 1.0)
F32 = jnp.float32
BF16 = jnp.bfloat16
VMEM = pl.BlockSpec(memory_space=pltpu.VMEM)
SMEM = pl.BlockSpec(memory_space=pltpu.SMEM)
EXTRA = 8
STEPS = 4
VMEM_LIMIT = 12 * 2**20


def split(value):
    high = value.astype(BF16)
    return high, (value - high.astype(F32)).astype(BF16)


def pack_kernel(steps, x_ref, *refs):
    me = lax.axis_index("amp")
    out_refs, held, sems = refs[:-2], refs[-2], refs[-1]
    register, middle, lanes = held.shape
    step = register // steps
    copies = []
    for at in range(steps):
        span = pl.ds(at * step, step)
        copies.append(pltpu.make_async_copy(x_ref.at[span, 0:middle, :], held.at[span], sems.at[at]))
        copies[-1].start()
    rows = held.reshape(register * middle, lanes)
    for at in range(steps):
        copies[at].wait()
        for far, out in enumerate(out_refs):
            for near in range(2):
                first = at * step * middle + (me ^ (2 * far + near))
                out[near, at * step : (at + 1) * step, :] = rows[pl.ds(first, step, stride=middle), :]


def pack_both_kernel(x_ref, side_ref, *out_refs):
    me = lax.axis_index("amp")
    register, middle, lanes = x_ref.shape
    for near, ref in enumerate((x_ref, side_ref)):
        rows = ref.reshape(register * middle, lanes)
        for far, out in enumerate(out_refs):
            out[near] = rows[pl.ds(me ^ (2 * far), register, stride=middle), :]


def part_kernel(*refs):
    lines = len(refs) - 2
    for far in range(lines):
        refs[lines][far] = refs[far][0]
        refs[lines + 1][far] = refs[far][1]


def part_last_kernel(piece_ref, near_ref, other_ref):
    register = near_ref.shape[1]
    sums = piece_ref[2 * register :, :]
    for near, out in enumerate((near_ref, other_ref)):
        out[:register, :] = piece_ref[near * register : (near + 1) * register, :]
        out[register:, :] = sums


def join_kernel(own_ref, other_ref, *out_refs):
    register = own_ref.shape[1]
    last = len(out_refs) * register
    sums = own_ref[last:, :] + other_ref[last:, :]
    for far, out in enumerate(out_refs):
        for near, ref in enumerate((own_ref, other_ref)):
            out[near * register : (near + 1) * register, :] = ref[far * register : (far + 1) * register, :]
        out[2 * register :, :] = sums


def pick_of(pick, factors):
    value = jnp.float32(factors[-1])
    for option in range(len(factors) - 1):
        value = jnp.where(pick == option, factors[option], value)
    return value


def noise_rows(picks_ref, section, block, register):
    rows = lax.broadcasted_iota(jnp.int32, (register, register), 0)
    product = jnp.ones((register, register), F32)
    qubits = picks_ref.shape[-1]
    for q in range(qubits):
        pick = picks_ref[section, block, q]
        bit = jnp.right_shift(rows, qubits - 1 - q) & 1
        product = product * jnp.where(bit == 1, pick_of(pick, FLIP_FACTORS), pick_of(pick, KEEP_FACTORS))
    return product


def combine_kernel(sections, picks_ref, targets_ref, *refs):
    gate_refs, (low_ref, high_ref) = refs[:sections], refs[sections:]
    seg = lax.axis_index("segment")
    blocks, register = gate_refs[0].shape[0], gate_refs[0].shape[-1]
    rows = lax.broadcasted_iota(jnp.int32, (register, register), 0)
    columns = lax.broadcasted_iota(jnp.int32, (register, register), 1)
    eye = (rows == columns).astype(F32)
    zero = jnp.zeros((register, register), BF16)
    for k in range(sections):
        section = seg ^ k
        low, high = eye, eye
        for block in range(blocks):
            on_low = targets_ref[section, block] == 0
            moved = gate_refs[k][block] * noise_rows(picks_ref, section, block, register)
            if block > 0:
                before = jnp.where(on_low, low, high)
                moved = jnp.dot(moved, before, precision=lax.Precision.HIGHEST, preferred_element_type=F32)
            low, high = jnp.where(on_low, moved, low), jnp.where(on_low, high, moved)
        big, small = split(low.T)
        low_ref[section] = jnp.concatenate(
            [jnp.concatenate([big, small], axis=1), jnp.concatenate([big, zero], axis=1)], axis=0
        )
        big, small = split(high)
        high_ref[section] = jnp.concatenate(
            [jnp.concatenate([big, big], axis=1), jnp.concatenate([small, zero], axis=1)], axis=0
        )


def on_low(value, weights):
    lanes = value.shape[1]
    both = jnp.dot(jnp.concatenate(split(value), axis=1), weights, preferred_element_type=F32)
    return both[:, :lanes] + both[:, lanes:]


def on_high(value, weights):
    rows = value.shape[0] // 2
    wide = jnp.concatenate([value[:rows], value[rows:]], axis=1)
    both = jnp.dot(weights, jnp.concatenate(split(wide), axis=0), preferred_element_type=F32)
    both = both[:rows] + both[rows:]
    lanes = value.shape[1]
    return jnp.concatenate([both[:, :lanes], both[:, lanes:]], axis=0)


def piece_of(refs, far, near):
    return refs[near].at[far] if len(refs) == 2 else refs[far].at[near]


def sections_kernel(sections, lines, pieces, last, *refs):
    amp = 2 * lines
    piece_refs, (low_ref, high_ref) = refs[:pieces], refs[pieces : pieces + 2]
    at = pieces + 2
    if last:
        sums_in, at = refs[at], at + 1
    out_refs, x = refs[at:-1], refs[-1]
    me = lax.axis_index("amp")
    register, lanes = piece_refs[0].shape[-2:]
    rest = register // amp

    def squares(total, value):
        return total + jnp.sum(value * value, axis=0, keepdims=True)

    total = jnp.zeros((1, lanes), F32)
    for far in range(lines):
        for near in range(2):
            value = piece_of(piece_refs, far, near)[...]
            total = squares(total, value)
            x[me ^ (2 * far + near)] = value
    sums = [total]
    for section in range(sections):
        low, high = low_ref[section], high_ref[section]
        total = jnp.zeros((1, lanes), F32)
        for pair in range(lines):
            parts = (2 * pair, 2 * pair + 1)
            if section % 2 == 0:
                value = jnp.concatenate([x[part] for part in parts], axis=0)
            else:
                spans = [x[:, part * rest : (part + 1) * rest, :].reshape(register, lanes) for part in parts]
                value = jnp.concatenate(spans, axis=0)
            value = on_high(on_low(value, low), high)
            total = squares(total, value)
            for half, part in enumerate(parts):
                piece = value[half * register : (half + 1) * register]
                if section % 2 == 0:
                    x[part] = piece
                else:
                    x[:, part * rest : (part + 1) * rest, :] = piece.reshape(amp, rest, lanes)
        sums.append(total)
    rows = jnp.concatenate(sums + [jnp.zeros((EXTRA - len(sums), lanes), F32)], axis=0)
    if not last:
        for far in range(lines):
            for near in range(2):
                out_refs[far][near] = x[me ^ (2 * far + near)]
        out_refs[lines][...] = rows
        return
    rows = rows + sums_in[...]
    first = out_refs[0]
    for near in range(2):
        first[near * register : (near + 1) * register, :] = x[me ^ (2 * (lines - 1) + near)]
        for far in range(lines - 1):
            out_refs[1 + near][far * register : (far + 1) * register, :] = x[me ^ (2 * far + near)]
        out_refs[1 + near][(lines - 1) * register :, :] = rows
    first[2 * register :, :] = rows


def unpack_kernel(lines, early, steps, total_amps, *refs):
    held, refs = refs[: 2 * early], refs[2 * early :]
    joined, far_refs, (x_ref, logs_ref, out, sems) = refs[: lines - 1], refs[lines - 1 : lines + 1], refs[lines + 1 :]
    me = lax.axis_index("amp")
    register, middle, lanes = out.shape
    sections = logs_ref.shape[1]
    totals = far_refs[0][register:, :] + far_refs[1][register:, :]
    for ref in joined:
        totals = totals + ref[2 * register :, :]
    totals = jnp.sum(totals, axis=1, keepdims=True)
    scale = 1.0 / jnp.sqrt(totals[sections : sections + 1] / total_amps)
    flat = out.reshape(register * middle, lanes)
    step = register // steps
    copies = []
    for at in range(steps):
        low, high = at * step, (at + 1) * step
        for chunk in range(early + 1):
            for far in range(lines):
                for near in range(2):
                    if chunk < early:
                        value = held[2 * chunk + near][far, low:high, :]
                    elif far < lines - 1:
                        value = joined[far][near * register + low : near * register + high, :]
                    else:
                        value = far_refs[near][low:high, :]
                    m = chunk * 2 * lines + (me ^ (2 * far + near))
                    flat[pl.ds(low * middle + m, step, stride=middle), :] = value * scale
        span = pl.ds(low, step)
        copies.append(pltpu.make_async_copy(out.at[span], x_ref.at[span], sems.at[at]))
        copies[-1].start()
    logs = jnp.log(totals[1 : sections + 1] / totals[:sections])
    rows = lax.broadcasted_iota(jnp.int32, (sections, sections), 0)
    columns = lax.broadcasted_iota(jnp.int32, (sections, sections), 1)
    logs_ref[...] = jnp.sum(jnp.where(rows == columns, logs, 0.0), axis=0, keepdims=True)
    for copy in copies:
        copy.wait()


def swap(piece, k, size, axis):
    if k == 0:
        return piece
    return lax.ppermute(piece, axis, [(i, i ^ k) for i in range(size)])


def body_fast(states, gate_blocks, kraus_picks, block_targets):
    amp_local = states.shape[1]
    register = gate_blocks.shape[-1]
    amp, sections = lax.axis_size("amp"), lax.axis_size("segment")
    middle = amp_local // (register * register)
    chunks, lines = middle // amp, amp // 2
    params = pltpu.CompilerParams(vmem_limit_bytes=VMEM_LIMIT)

    def array(*shape, dtype=F32):
        return jax.ShapeDtypeStruct(shape, dtype)

    def kernel(body, out_shape, *operands, **options):
        specs = dict(in_specs=[VMEM] * len(operands), out_specs=[VMEM] * len(out_shape))
        return pl.pallas_call(body, out_shape=out_shape, compiler_params=params, **{**specs, **options})(*operands)

    def along(pieces):
        count = len(pieces)
        back = {far: swap(pieces[far], 2 * far, amp, "amp") for far in range(count - 1, -1, -1)}
        return [back[far] for far in range(count)]

    def across(piece):
        return swap(piece, 1, amp, "amp")

    pairs, halves = [array(2, register, register)] * lines, [array(lines, register, register)] * 2
    x = states.reshape(register, middle, register)
    arrived = []
    for chunk in range(chunks):
        if chunk == 0:
            packed = kernel(
                functools.partial(pack_kernel, STEPS),
                pairs,
                pltpu.with_memory_space_constraint(x, pltpu.HBM),
                in_specs=[pl.BlockSpec(memory_space=pltpu.HBM)],
                scratch_shapes=[pltpu.VMEM((register, amp, register), F32), pltpu.SemaphoreType.DMA((STEPS,))],
            )
            near, other = kernel(part_kernel, halves, *along(packed))
            arrived.append([near, across(other)])
        else:
            own = x[:, chunk * amp : (chunk + 1) * amp, :]
            packed = kernel(pack_both_kernel, pairs, own, across(own))
            arrived.append(along(packed))

    gates = [swap(gate_blocks[0], k, sections, "segment") for k in range(sections)]
    low, high = kernel(
        functools.partial(combine_kernel, sections),
        [array(sections, 2 * register, 2 * register, dtype=BF16)] * 2,
        kraus_picks[0],
        block_targets,
        *gates,
        in_specs=[SMEM, SMEM] + [VMEM] * sections,
    )

    carried, held = [], []
    for chunk, pieces in enumerate(arrived):
        last = chunk == chunks - 1
        both = 2 * register + EXTRA
        aside = array((lines - 1) * register + EXTRA, register)
        results = kernel(
            functools.partial(sections_kernel, sections, lines, len(pieces), last),
            [array(both, register), aside, aside] if last else pairs + [array(EXTRA, register)],
            *pieces,
            low,
            high,
            *carried,
            scratch_shapes=[pltpu.VMEM((amp, register, register), F32)],
        )
        if last:
            first, own, other = results
            first = swap(first, 2 * (lines - 1), amp, "amp")
            tall = [array(both, register)] * (lines - 1)
            held += along(kernel(join_kernel, tall, own, across(other)))
            tall = [array(register + EXTRA, register)] * 2
            near, other = kernel(part_last_kernel, tall, first)
            held += [near, across(other)]
        else:
            carried = [results[lines]]
            near, other = kernel(part_kernel, halves, *along(results[:lines]))
            held += [near, across(other)]

    out, logs = kernel(
        functools.partial(unpack_kernel, lines, chunks - 1, STEPS, float(amp_local * amp)),
        [array(register, middle, register), array(1, sections)],
        *held,
        out_specs=[pl.BlockSpec(memory_space=pltpu.HBM), VMEM],
        scratch_shapes=[pltpu.VMEM((register, middle, register), F32), pltpu.SemaphoreType.DMA((STEPS,))],
    )
    return out.reshape(1, amp_local), logs


def noise_factors(kraus_rows):
    qubit_count = kraus_rows.shape[-1]
    register = 2**qubit_count
    positions = jnp.arange(register, dtype=jnp.int32)
    product = jnp.ones(kraus_rows.shape[:-1] + (register,), jnp.float32)
    for qubit_pos in range(qubit_count):
        bit_value = jnp.right_shift(positions, qubit_count - 1 - qubit_pos) & 1
        column = kraus_rows[..., qubit_pos : qubit_pos + 1]
        low_value = jnp.zeros(column.shape, jnp.float32)
        high_value = jnp.zeros(column.shape, jnp.float32)
        for option in range(4):
            picked = (column == option).astype(jnp.float32)
            low_value = low_value + picked * KEEP_FACTORS[option]
            high_value = high_value + picked * FLIP_FACTORS[option]
        product = product * jnp.where(bit_value == 1, high_value, low_value)
    return product


def apply_gate(amplitudes, matrix, factors, target):

    def on_low(values):
        mixed_rows = jnp.einsum("bhmk,ik->bhmi", values, matrix, precision=lax.Precision.HIGHEST)
        return mixed_rows * factors[:, None, None, :]

    def on_high(values):
        mixed_rows = jnp.einsum("bjmk,ij->bimk", values, matrix, precision=lax.Precision.HIGHEST)
        return mixed_rows * factors[:, :, None, None]

    return lax.cond(target == 0, on_low, on_high, amplitudes)


def square_sums(values):
    return (values, jnp.sum(values * values, axis=(1, 2, 3)))


def body_general(states, gate_blocks, kraus_picks, block_targets):
    traj_here = states.shape[0]
    amp_local = states.shape[1]
    register = gate_blocks.shape[-1]
    blocks = gate_blocks.shape[1]
    middle = amp_local // (register * register)
    total_amps = amp_local * lax.axis_size("amp")
    sections = lax.axis_size("segment")
    amplitudes = states.reshape(traj_here, register, middle, register)
    local_sums = [jnp.sum(amplitudes * amplitudes, axis=(1, 2, 3))]
    for section in range(sections):
        owned = jnp.where(lax.axis_index("segment") == section, gate_blocks, jnp.zeros_like(gate_blocks))
        section_gates = lax.psum(owned, "segment")[0]
        for block_pos in range(blocks):
            factors = noise_factors(kraus_picks[:, section, block_pos, :])
            amplitudes = apply_gate(
                amplitudes, section_gates[block_pos], factors, block_targets[section, block_pos]
            )
        amplitudes, local_sq = square_sums(
            lax.all_to_all(amplitudes, "amp", split_axis=1, concat_axis=1, tiled=True)
        )
        local_sums.append(local_sq)
    totals = lax.psum(jnp.stack(local_sums, axis=1), "amp")
    log_weights = jnp.log(totals[:, 1:] / totals[:, :-1])
    amplitudes = amplitudes / jnp.sqrt(totals[:, -1] / total_amps)[:, None, None, None]
    return (amplitudes.reshape(traj_here, amp_local), log_weights)


def solution(mesh):
    in_specs = (
        P("segment", "amp"),
        P("segment", None, None, None),
        P("segment", None, None, None),
        P(),
    )
    out_specs = (P("segment", "amp"), P("segment", None))
    amp, sections = mesh.shape["amp"], mesh.shape["segment"]

    def run(states, gate_blocks, kraus_picks, block_targets):
        register = gate_blocks.shape[-1]
        middle = states.shape[1] // amp // (register * register)
        power_of_two = amp > 2 and amp & (amp - 1) == 0 and sections & (sections - 1) == 0
        fits = middle > 0 and middle % amp == 0 and register % (8 * amp) == 0
        fast = power_of_two and fits and sections % 2 == 0 and sections < EXTRA and states.shape[0] == sections

        def body(*args):
            return (body_fast if fast else body_general)(*args)

        step = jax.shard_map(body, mesh=mesh, in_specs=in_specs, out_specs=out_specs, check_vma=False)
        return step(states, gate_blocks, kraus_picks, block_targets)

    return run
```

```python
import functools

import jax
import jax.numpy as jnp
from jax import lax
from jax.experimental import pallas as pl
from jax.experimental.pallas import tpu as pltpu
from jax.sharding import PartitionSpec as P


KEEP_FACTORS = (1.0, 0.9, 1.0, 0.97)
FLIP_FACTORS = (0.9, 1.0, 0.97, 1.0)
F32 = jnp.float32
BF16 = jnp.bfloat16
VMEM = pl.BlockSpec(memory_space=pltpu.VMEM)
SMEM = pl.BlockSpec(memory_space=pltpu.SMEM)
EXTRA = 8
STEPS = 4
OUT_STEPS = 8
VMEM_LIMIT = 12 * 2**20


def split(value):
    high = value.astype(BF16)
    return high, (value - high.astype(F32)).astype(BF16)


def pack_kernel(steps, x_ref, *refs):
    me = lax.axis_index("amp")
    out_refs, held, sems = refs[:-2], refs[-2], refs[-1]
    register, middle, lanes = held.shape
    step = register // steps
    copies = []
    for at in range(steps):
        span = pl.ds(at * step, step)
        copies.append(pltpu.make_async_copy(x_ref.at[span, 0:middle, :], held.at[span], sems.at[at]))
        copies[-1].start()
    rows = held.reshape(register * middle, lanes)
    for at in range(steps):
        copies[at].wait()
        for far, out in enumerate(out_refs):
            for near in range(2):
                first = at * step * middle + (me ^ (2 * far + near))
                out[near, at * step : (at + 1) * step, :] = rows[pl.ds(first, step, stride=middle), :]


def pack_both_kernel(x_ref, side_ref, *out_refs):
    me = lax.axis_index("amp")
    register, middle, lanes = x_ref.shape
    for near, ref in enumerate((x_ref, side_ref)):
        rows = ref.reshape(register * middle, lanes)
        for far, out in enumerate(out_refs):
            out[near] = rows[pl.ds(me ^ (2 * far), register, stride=middle), :]


def part_kernel(*refs):
    lines = len(refs) - 2
    for far in range(lines):
        refs[lines][far] = refs[far][0]
        refs[lines + 1][far] = refs[far][1]


def part_last_kernel(piece_ref, near_ref, other_ref):
    register = near_ref.shape[1]
    sums = piece_ref[2 * register :, :]
    for near, out in enumerate((near_ref, other_ref)):
        out[:register, :] = piece_ref[near * register : (near + 1) * register, :]
        out[register:, :] = sums


def join_kernel(own_ref, other_ref, *out_refs):
    register = own_ref.shape[1]
    last = len(out_refs) * register
    sums = own_ref[last:, :] + other_ref[last:, :]
    for far, out in enumerate(out_refs):
        for near, ref in enumerate((own_ref, other_ref)):
            out[near * register : (near + 1) * register, :] = ref[far * register : (far + 1) * register, :]
        out[2 * register :, :] = sums


def pick_of(pick, factors):
    value = jnp.float32(factors[-1])
    for option in range(len(factors) - 1):
        value = jnp.where(pick == option, factors[option], value)
    return value


def noise_rows(picks_ref, section, block, register):
    rows = lax.broadcasted_iota(jnp.int32, (register, register), 0)
    product = jnp.ones((register, register), F32)
    qubits = picks_ref.shape[-1]
    for q in range(qubits):
        pick = picks_ref[section, block, q]
        bit = jnp.right_shift(rows, qubits - 1 - q) & 1
        product = product * jnp.where(bit == 1, pick_of(pick, FLIP_FACTORS), pick_of(pick, KEEP_FACTORS))
    return product


def combine_kernel(sections, picks_ref, targets_ref, *refs):
    gate_refs, (low_ref, high_ref) = refs[:sections], refs[sections:]
    seg = lax.axis_index("segment")
    blocks, register = gate_refs[0].shape[0], gate_refs[0].shape[-1]
    rows = lax.broadcasted_iota(jnp.int32, (register, register), 0)
    columns = lax.broadcasted_iota(jnp.int32, (register, register), 1)
    eye = (rows == columns).astype(F32)
    zero = jnp.zeros((register, register), BF16)
    for k in range(sections):
        section = seg ^ k
        low, high = eye, eye
        for block in range(blocks):
            on_low = targets_ref[section, block] == 0
            moved = gate_refs[k][block] * noise_rows(picks_ref, section, block, register)
            if block > 0:
                before = jnp.where(on_low, low, high)
                moved = jnp.dot(moved, before, precision=lax.Precision.HIGHEST, preferred_element_type=F32)
            low, high = jnp.where(on_low, moved, low), jnp.where(on_low, high, moved)
        big, small = split(low.T)
        low_ref[section] = jnp.concatenate(
            [jnp.concatenate([big, small], axis=1), jnp.concatenate([big, zero], axis=1)], axis=0
        )
        big, small = split(high)
        high_ref[section] = jnp.concatenate(
            [jnp.concatenate([big, big], axis=1), jnp.concatenate([small, zero], axis=1)], axis=0
        )


def on_low(value, weights):
    lanes = value.shape[1]
    both = jnp.dot(jnp.concatenate(split(value), axis=1), weights, preferred_element_type=F32)
    return both[:, :lanes] + both[:, lanes:]


def on_high(value, weights):
    rows = value.shape[0] // 2
    wide = jnp.concatenate([value[:rows], value[rows:]], axis=1)
    both = jnp.dot(weights, jnp.concatenate(split(wide), axis=0), preferred_element_type=F32)
    both = both[:rows] + both[rows:]
    lanes = value.shape[1]
    return jnp.concatenate([both[:, :lanes], both[:, lanes:]], axis=0)


def piece_of(refs, far, near):
    return refs[near].at[far] if len(refs) == 2 else refs[far].at[near]


def sections_kernel(sections, lines, pieces, last, *refs):
    amp = 2 * lines
    piece_refs, (low_ref, high_ref) = refs[:pieces], refs[pieces : pieces + 2]
    at = pieces + 2
    if last:
        sums_in, at = refs[at], at + 1
    out_refs, x = refs[at:-1], refs[-1]
    me = lax.axis_index("amp")
    register, lanes = piece_refs[0].shape[-2:]
    rest = register // amp

    def squares(total, value):
        return total + jnp.sum(value * value, axis=0, keepdims=True)

    total = jnp.zeros((1, lanes), F32)
    for far in range(lines):
        for near in range(2):
            value = piece_of(piece_refs, far, near)[...]
            total = squares(total, value)
            x[me ^ (2 * far + near)] = value
    sums = [total]
    for section in range(sections):
        low, high = low_ref[section], high_ref[section]
        total = jnp.zeros((1, lanes), F32)
        for pair in range(lines):
            parts = (2 * pair, 2 * pair + 1)
            if section % 2 == 0:
                value = jnp.concatenate([x[part] for part in parts], axis=0)
            else:
                spans = [x[:, part * rest : (part + 1) * rest, :].reshape(register, lanes) for part in parts]
                value = jnp.concatenate(spans, axis=0)
            value = on_high(on_low(value, low), high)
            total = squares(total, value)
            for half, part in enumerate(parts):
                piece = value[half * register : (half + 1) * register]
                if section % 2 == 0:
                    x[part] = piece
                else:
                    x[:, part * rest : (part + 1) * rest, :] = piece.reshape(amp, rest, lanes)
        sums.append(total)
    rows = jnp.concatenate(sums + [jnp.zeros((EXTRA - len(sums), lanes), F32)], axis=0)
    if not last:
        for far in range(lines):
            for near in range(2):
                out_refs[far][near] = x[me ^ (2 * far + near)]
        out_refs[lines][...] = rows
        return
    rows = rows + sums_in[...]
    first = out_refs[0]
    for near in range(2):
        first[near * register : (near + 1) * register, :] = x[me ^ (2 * (lines - 1) + near)]
        for far in range(lines - 1):
            out_refs[1 + near][far * register : (far + 1) * register, :] = x[me ^ (2 * far + near)]
        out_refs[1 + near][(lines - 1) * register :, :] = rows
    first[2 * register :, :] = rows


def unpack_kernel(lines, early, steps, total_amps, *refs):
    held, refs = refs[: 2 * early], refs[2 * early :]
    joined, far_refs, (x_ref, logs_ref, out, logs_held, sems) = refs[: lines - 1], refs[lines - 1 : lines + 1], refs[lines + 1 :]
    me = lax.axis_index("amp")
    register, middle, lanes = out.shape
    sections = logs_ref.shape[1]
    totals = far_refs[0][register:, :] + far_refs[1][register:, :]
    for ref in joined:
        totals = totals + ref[2 * register :, :]
    totals = jnp.sum(totals, axis=1, keepdims=True)
    scale = 1.0 / jnp.sqrt(totals[sections : sections + 1] / total_amps)
    flat = out.reshape(register * middle, lanes)
    step = register // steps
    copies = []
    for at in range(steps):
        low, high = at * step, (at + 1) * step
        for chunk in range(early + 1):
            for far in range(lines):
                for near in range(2):
                    if chunk < early:
                        value = held[2 * chunk + near][far, low:high, :]
                    elif far < lines - 1:
                        value = joined[far][near * register + low : near * register + high, :]
                    else:
                        value = far_refs[near][low:high, :]
                    m = chunk * 2 * lines + (me ^ (2 * far + near))
                    flat[pl.ds(low * middle + m, step, stride=middle), :] = value * scale
        span = pl.ds(low, step)
        copies.append(pltpu.make_async_copy(out.at[span], x_ref.at[span], sems.at[at]))
        copies[-1].start()
    logs = jnp.log(totals[1 : sections + 1] / totals[:sections])
    rows = lax.broadcasted_iota(jnp.int32, (sections, sections), 0)
    columns = lax.broadcasted_iota(jnp.int32, (sections, sections), 1)
    logs_held[...] = jnp.sum(jnp.where(rows == columns, logs, 0.0), axis=0, keepdims=True)
    copies.append(pltpu.make_async_copy(logs_held, logs_ref, sems.at[steps]))
    copies[-1].start()
    for copy in copies:
        copy.wait()


def swap(piece, k, size, axis):
    if k == 0:
        return piece
    return lax.ppermute(piece, axis, [(i, i ^ k) for i in range(size)])


def body_fast(states, gate_blocks, kraus_picks, block_targets):
    amp_local = states.shape[1]
    register = gate_blocks.shape[-1]
    amp, sections = lax.axis_size("amp"), lax.axis_size("segment")
    middle = amp_local // (register * register)
    chunks, lines = middle // amp, amp // 2
    params = pltpu.CompilerParams(vmem_limit_bytes=VMEM_LIMIT)

    def array(*shape, dtype=F32):
        return jax.ShapeDtypeStruct(shape, dtype)

    def kernel(body, out_shape, *operands, **options):
        specs = dict(in_specs=[VMEM] * len(operands), out_specs=[VMEM] * len(out_shape))
        return pl.pallas_call(body, out_shape=out_shape, compiler_params=params, **{**specs, **options})(*operands)

    def along(pieces):
        count = len(pieces)
        back = {far: swap(pieces[far], 2 * far, amp, "amp") for far in range(count - 1, -1, -1)}
        return [back[far] for far in range(count)]

    def across(piece):
        return swap(piece, 1, amp, "amp")

    pairs, halves = [array(2, register, register)] * lines, [array(lines, register, register)] * 2
    x = states.reshape(register, middle, register)
    arrived = []
    for chunk in range(chunks):
        if chunk == 0:
            packed = kernel(
                functools.partial(pack_kernel, STEPS),
                pairs,
                pltpu.with_memory_space_constraint(x, pltpu.HBM),
                in_specs=[pl.BlockSpec(memory_space=pltpu.HBM)],
                scratch_shapes=[pltpu.VMEM((register, amp, register), F32), pltpu.SemaphoreType.DMA((STEPS,))],
            )
            near, other = kernel(part_kernel, halves, *along(packed))
            arrived.append([near, across(other)])
        else:
            own = x[:, chunk * amp : (chunk + 1) * amp, :]
            packed = kernel(pack_both_kernel, pairs, own, across(own))
            arrived.append(along(packed))

    gates = [swap(gate_blocks[0], k, sections, "segment") for k in range(sections)]
    low, high = kernel(
        functools.partial(combine_kernel, sections),
        [array(sections, 2 * register, 2 * register, dtype=BF16)] * 2,
        kraus_picks[0],
        block_targets,
        *gates,
        in_specs=[SMEM, SMEM] + [VMEM] * sections,
    )

    carried, held = [], []
    for chunk, pieces in enumerate(arrived):
        last = chunk == chunks - 1
        both = 2 * register + EXTRA
        aside = array((lines - 1) * register + EXTRA, register)
        results = kernel(
            functools.partial(sections_kernel, sections, lines, len(pieces), last),
            [array(both, register), aside, aside] if last else pairs + [array(EXTRA, register)],
            *pieces,
            low,
            high,
            *carried,
            scratch_shapes=[pltpu.VMEM((amp, register, register), F32)],
        )
        if last:
            first, own, other = results
            first = swap(first, 2 * (lines - 1), amp, "amp")
            tall = [array(both, register)] * (lines - 1)
            held += along(kernel(join_kernel, tall, own, across(other)))
            tall = [array(register + EXTRA, register)] * 2
            near, other = kernel(part_last_kernel, tall, first)
            held += [near, across(other)]
        else:
            carried = [results[lines]]
            near, other = kernel(part_kernel, halves, *along(results[:lines]))
            held += [near, across(other)]

    out, logs = kernel(
        functools.partial(unpack_kernel, lines, chunks - 1, OUT_STEPS, float(amp_local * amp)),
        [array(register, middle, register), array(1, sections)],
        *held,
        out_specs=[pl.BlockSpec(memory_space=pltpu.HBM)] * 2,
        scratch_shapes=[
            pltpu.VMEM((register, middle, register), F32),
            pltpu.VMEM((1, sections), F32),
            pltpu.SemaphoreType.DMA((OUT_STEPS + 1,)),
        ],
    )
    return out.reshape(1, amp_local), logs


def noise_factors(kraus_rows):
    qubit_count = kraus_rows.shape[-1]
    register = 2**qubit_count
    positions = jnp.arange(register, dtype=jnp.int32)
    product = jnp.ones(kraus_rows.shape[:-1] + (register,), jnp.float32)
    for qubit_pos in range(qubit_count):
        bit_value = jnp.right_shift(positions, qubit_count - 1 - qubit_pos) & 1
        column = kraus_rows[..., qubit_pos : qubit_pos + 1]
        low_value = jnp.zeros(column.shape, jnp.float32)
        high_value = jnp.zeros(column.shape, jnp.float32)
        for option in range(4):
            picked = (column == option).astype(jnp.float32)
            low_value = low_value + picked * KEEP_FACTORS[option]
            high_value = high_value + picked * FLIP_FACTORS[option]
        product = product * jnp.where(bit_value == 1, high_value, low_value)
    return product


def apply_gate(amplitudes, matrix, factors, target):

    def on_low(values):
        mixed_rows = jnp.einsum("bhmk,ik->bhmi", values, matrix, precision=lax.Precision.HIGHEST)
        return mixed_rows * factors[:, None, None, :]

    def on_high(values):
        mixed_rows = jnp.einsum("bjmk,ij->bimk", values, matrix, precision=lax.Precision.HIGHEST)
        return mixed_rows * factors[:, :, None, None]

    return lax.cond(target == 0, on_low, on_high, amplitudes)


def square_sums(values):
    return (values, jnp.sum(values * values, axis=(1, 2, 3)))


def body_general(states, gate_blocks, kraus_picks, block_targets):
    traj_here = states.shape[0]
    amp_local = states.shape[1]
    register = gate_blocks.shape[-1]
    blocks = gate_blocks.shape[1]
    middle = amp_local // (register * register)
    total_amps = amp_local * lax.axis_size("amp")
    sections = lax.axis_size("segment")
    amplitudes = states.reshape(traj_here, register, middle, register)
    local_sums = [jnp.sum(amplitudes * amplitudes, axis=(1, 2, 3))]
    for section in range(sections):
        owned = jnp.where(lax.axis_index("segment") == section, gate_blocks, jnp.zeros_like(gate_blocks))
        section_gates = lax.psum(owned, "segment")[0]
        for block_pos in range(blocks):
            factors = noise_factors(kraus_picks[:, section, block_pos, :])
            amplitudes = apply_gate(
                amplitudes, section_gates[block_pos], factors, block_targets[section, block_pos]
            )
        amplitudes, local_sq = square_sums(
            lax.all_to_all(amplitudes, "amp", split_axis=1, concat_axis=1, tiled=True)
        )
        local_sums.append(local_sq)
    totals = lax.psum(jnp.stack(local_sums, axis=1), "amp")
    log_weights = jnp.log(totals[:, 1:] / totals[:, :-1])
    amplitudes = amplitudes / jnp.sqrt(totals[:, -1] / total_amps)[:, None, None, None]
    return (amplitudes.reshape(traj_here, amp_local), log_weights)


def solution(mesh):
    in_specs = (
        P("segment", "amp"),
        P("segment", None, None, None),
        P("segment", None, None, None),
        P(),
    )
    out_specs = (P("segment", "amp"), P("segment", None))
    amp, sections = mesh.shape["amp"], mesh.shape["segment"]

    def run(states, gate_blocks, kraus_picks, block_targets):
        register = gate_blocks.shape[-1]
        middle = states.shape[1] // amp // (register * register)
        power_of_two = amp > 2 and amp & (amp - 1) == 0 and sections & (sections - 1) == 0
        fits = middle > 0 and middle % amp == 0 and register % (8 * amp) == 0
        fast = power_of_two and fits and sections % 2 == 0 and sections < EXTRA and states.shape[0] == sections

        def body(*args):
            return (body_fast if fast else body_general)(*args)

        step = jax.shard_map(body, mesh=mesh, in_specs=in_specs, out_specs=out_specs, check_vma=False)
        return step(states, gate_blocks, kraus_picks, block_targets)

    return run
```

```python
import functools

import jax
import jax.numpy as jnp
from jax import lax
from jax.experimental import pallas as pl
from jax.experimental.pallas import tpu as pltpu
from jax.sharding import PartitionSpec as P


KEEP_FACTORS = (1.0, 0.9, 1.0, 0.97)
FLIP_FACTORS = (0.9, 1.0, 0.97, 1.0)
F32 = jnp.float32
BF16 = jnp.bfloat16
VMEM = pl.BlockSpec(memory_space=pltpu.VMEM)
SMEM = pl.BlockSpec(memory_space=pltpu.SMEM)
EXTRA = 8
STEPS = 4
OUT_STEPS = 8
IN_WAYS = (0, 0)
OUT_WAYS = (0, 1)
VMEM_LIMIT = 12 * 2**20


def device_at(me, step, near, lines, way):
    line = (me // 2) ^ step if way == 0 else (me // 2 + way * step) & (lines - 1)
    return 2 * line + ((me % 2) ^ near)


def split(value):
    high = value.astype(BF16)
    return high, (value - high.astype(F32)).astype(BF16)


def pack_kernel(steps, way, x_ref, *refs):
    me = lax.axis_index("amp")
    out_refs, held, sems = refs[:-2], refs[-2], refs[-1]
    register, middle, lanes = held.shape
    step = register // steps
    copies = []
    for at in range(steps):
        span = pl.ds(at * step, step)
        copies.append(pltpu.make_async_copy(x_ref.at[span, 0:middle, :], held.at[span], sems.at[at]))
        copies[-1].start()
    rows = held.reshape(register * middle, lanes)
    for at in range(steps):
        copies[at].wait()
        for far, out in enumerate(out_refs):
            for near in range(2):
                first = at * step * middle + device_at(me, far, near, len(out_refs), way)
                out[near, at * step : (at + 1) * step, :] = rows[pl.ds(first, step, stride=middle), :]


def pack_both_kernel(way, x_ref, side_ref, *out_refs):
    me = lax.axis_index("amp")
    register, middle, lanes = x_ref.shape
    for near, ref in enumerate((x_ref, side_ref)):
        rows = ref.reshape(register * middle, lanes)
        for far, out in enumerate(out_refs):
            out[near] = rows[pl.ds(device_at(me, far, 0, len(out_refs), way), register, stride=middle), :]


def part_kernel(*refs):
    lines = len(refs) - 2
    for far in range(lines):
        refs[lines][far] = refs[far][0]
        refs[lines + 1][far] = refs[far][1]


def part_last_kernel(piece_ref, near_ref, other_ref):
    register = near_ref.shape[1]
    sums = piece_ref[2 * register :, :]
    for near, out in enumerate((near_ref, other_ref)):
        out[:register, :] = piece_ref[near * register : (near + 1) * register, :]
        out[register:, :] = sums


def join_kernel(own_ref, other_ref, *out_refs):
    register = own_ref.shape[1]
    last = len(out_refs) * register
    sums = own_ref[last:, :] + other_ref[last:, :]
    for far, out in enumerate(out_refs):
        for near, ref in enumerate((own_ref, other_ref)):
            out[near * register : (near + 1) * register, :] = ref[far * register : (far + 1) * register, :]
        out[2 * register :, :] = sums


def pick_of(pick, factors):
    value = jnp.float32(factors[-1])
    for option in range(len(factors) - 1):
        value = jnp.where(pick == option, factors[option], value)
    return value


def noise_rows(picks_ref, section, block, register):
    rows = lax.broadcasted_iota(jnp.int32, (register, register), 0)
    product = jnp.ones((register, register), F32)
    qubits = picks_ref.shape[-1]
    for q in range(qubits):
        pick = picks_ref[section, block, q]
        bit = jnp.right_shift(rows, qubits - 1 - q) & 1
        product = product * jnp.where(bit == 1, pick_of(pick, FLIP_FACTORS), pick_of(pick, KEEP_FACTORS))
    return product


def combine_kernel(sections, picks_ref, targets_ref, *refs):
    gate_refs, (low_ref, high_ref) = refs[:sections], refs[sections:]
    seg = lax.axis_index("segment")
    blocks, register = gate_refs[0].shape[0], gate_refs[0].shape[-1]
    rows = lax.broadcasted_iota(jnp.int32, (register, register), 0)
    columns = lax.broadcasted_iota(jnp.int32, (register, register), 1)
    eye = (rows == columns).astype(F32)
    zero = jnp.zeros((register, register), BF16)
    for k in range(sections):
        section = seg ^ k
        low, high = eye, eye
        for block in range(blocks):
            on_low = targets_ref[section, block] == 0
            moved = gate_refs[k][block] * noise_rows(picks_ref, section, block, register)
            if block > 0:
                before = jnp.where(on_low, low, high)
                moved = jnp.dot(moved, before, precision=lax.Precision.HIGHEST, preferred_element_type=F32)
            low, high = jnp.where(on_low, moved, low), jnp.where(on_low, high, moved)
        big, small = split(low.T)
        low_ref[section] = jnp.concatenate(
            [jnp.concatenate([big, small], axis=1), jnp.concatenate([big, zero], axis=1)], axis=0
        )
        big, small = split(high)
        high_ref[section] = jnp.concatenate(
            [jnp.concatenate([big, big], axis=1), jnp.concatenate([small, zero], axis=1)], axis=0
        )


def on_low(value, weights):
    lanes = value.shape[1]
    both = jnp.dot(jnp.concatenate(split(value), axis=1), weights, preferred_element_type=F32)
    return both[:, :lanes] + both[:, lanes:]


def on_high(value, weights):
    rows = value.shape[0] // 2
    wide = jnp.concatenate([value[:rows], value[rows:]], axis=1)
    both = jnp.dot(weights, jnp.concatenate(split(wide), axis=0), preferred_element_type=F32)
    both = both[:rows] + both[rows:]
    lanes = value.shape[1]
    return jnp.concatenate([both[:, :lanes], both[:, lanes:]], axis=0)


def piece_of(refs, far, near):
    return refs[near].at[far] if len(refs) == 2 else refs[far].at[near]


def later_turns(lines):
    return [turn for turn in range(lines) if turn != 1]


def sections_kernel(sections, lines, ways, pieces, last, *refs):
    amp = 2 * lines
    piece_refs, (low_ref, high_ref) = refs[:pieces], refs[pieces : pieces + 2]
    at = pieces + 2
    if last:
        sums_in, at = refs[at], at + 1
    out_refs, x = refs[at:-1], refs[-1]
    me = lax.axis_index("amp")
    register, lanes = piece_refs[0].shape[-2:]
    rest = register // amp

    def squares(total, value):
        return total + jnp.sum(value * value, axis=0, keepdims=True)

    total = jnp.zeros((1, lanes), F32)
    for far in range(lines):
        for near in range(2):
            value = piece_of(piece_refs, far, near)[...]
            total = squares(total, value)
            x[device_at(me, far, near, lines, -ways[0])] = value
    sums = [total]
    for section in range(sections):
        low, high = low_ref[section], high_ref[section]
        total = jnp.zeros((1, lanes), F32)
        for pair in range(lines):
            parts = (2 * pair, 2 * pair + 1)
            if section % 2 == 0:
                value = jnp.concatenate([x[part] for part in parts], axis=0)
            else:
                spans = [x[:, part * rest : (part + 1) * rest, :].reshape(register, lanes) for part in parts]
                value = jnp.concatenate(spans, axis=0)
            value = on_high(on_low(value, low), high)
            total = squares(total, value)
            for half, part in enumerate(parts):
                piece = value[half * register : (half + 1) * register]
                if section % 2 == 0:
                    x[part] = piece
                else:
                    x[:, part * rest : (part + 1) * rest, :] = piece.reshape(amp, rest, lanes)
        sums.append(total)
    rows = jnp.concatenate(sums + [jnp.zeros((EXTRA - len(sums), lanes), F32)], axis=0)
    if not last:
        for far in range(lines):
            for near in range(2):
                out_refs[far][near] = x[device_at(me, far, near, lines, ways[1])]
        out_refs[lines][...] = rows
        return
    rows = rows + sums_in[...]
    first = out_refs[0]
    for near in range(2):
        first[near * register : (near + 1) * register, :] = x[device_at(me, 1, near, lines, ways[1])]
        for at, far in enumerate(later_turns(lines)):
            out_refs[1 + near][at * register : (at + 1) * register, :] = x[device_at(me, far, near, lines, ways[1])]
        out_refs[1 + near][(lines - 1) * register :, :] = rows
    first[2 * register :, :] = rows


def unpack_kernel(lines, ways, early, steps, total_amps, *refs):
    held, refs = refs[: 2 * early], refs[2 * early :]
    joined, first_refs, (x_ref, logs_ref, out, logs_held, sems) = refs[: lines - 1], refs[lines - 1 : lines + 1], refs[lines + 1 :]
    me = lax.axis_index("amp")
    register, middle, lanes = out.shape
    sections = logs_ref.shape[1]
    totals = first_refs[0][register:, :] + first_refs[1][register:, :]
    for ref in joined:
        totals = totals + ref[2 * register :, :]
    totals = jnp.sum(totals, axis=1, keepdims=True)
    scale = 1.0 / jnp.sqrt(totals[sections : sections + 1] / total_amps)
    flat = out.reshape(register * middle, lanes)
    step = register // steps
    copies = []
    for at in range(steps):
        low, high = at * step, (at + 1) * step
        for chunk in range(early + 1):
            for far in range(lines):
                for near in range(2):
                    if chunk < early:
                        value = held[2 * chunk + near][far, low:high, :]
                    else:
                        if far == 1:
                            value = first_refs[near][low:high, :]
                        else:
                            at_turn = later_turns(lines).index(far)
                            value = joined[at_turn][near * register + low : near * register + high, :]
                    m = chunk * 2 * lines + device_at(me, far, near, lines, -ways[chunk])
                    flat[pl.ds(low * middle + m, step, stride=middle), :] = value * scale
        span = pl.ds(low, step)
        copies.append(pltpu.make_async_copy(out.at[span], x_ref.at[span], sems.at[at]))
        copies[-1].start()
    logs = jnp.log(totals[1 : sections + 1] / totals[:sections])
    rows = lax.broadcasted_iota(jnp.int32, (sections, sections), 0)
    columns = lax.broadcasted_iota(jnp.int32, (sections, sections), 1)
    logs_held[...] = jnp.sum(jnp.where(rows == columns, logs, 0.0), axis=0, keepdims=True)
    copies.append(pltpu.make_async_copy(logs_held, logs_ref, sems.at[steps]))
    copies[-1].start()
    for copy in copies:
        copy.wait()


def swap(piece, k, size, axis):
    if k == 0:
        return piece
    return lax.ppermute(piece, axis, [(i, i ^ k) for i in range(size)])


def shift(piece, step, lines, way):
    if step == 0:
        return piece
    pairs = [(me, device_at(me, step, 0, lines, way)) for me in range(2 * lines)]
    return lax.ppermute(piece, "amp", pairs)


def body_fast(states, gate_blocks, kraus_picks, block_targets):
    amp_local = states.shape[1]
    register = gate_blocks.shape[-1]
    amp, sections = lax.axis_size("amp"), lax.axis_size("segment")
    middle = amp_local // (register * register)
    chunks, lines = middle // amp, amp // 2
    in_ways, out_ways = [IN_WAYS[chunk > 0] for chunk in range(chunks)], [OUT_WAYS[chunk == chunks - 1] for chunk in range(chunks)]
    params = pltpu.CompilerParams(vmem_limit_bytes=VMEM_LIMIT)

    def array(*shape, dtype=F32):
        return jax.ShapeDtypeStruct(shape, dtype)

    def kernel(body, out_shape, *operands, **options):
        specs = dict(in_specs=[VMEM] * len(operands), out_specs=[VMEM] * len(out_shape))
        return pl.pallas_call(body, out_shape=out_shape, compiler_params=params, **{**specs, **options})(*operands)

    def along(pieces, way):
        return [shift(piece, step, lines, way) for step, piece in enumerate(pieces)]

    def across(piece):
        return swap(piece, 1, amp, "amp")

    pairs, halves = [array(2, register, register)] * lines, [array(lines, register, register)] * 2
    x = states.reshape(register, middle, register)
    arrived = []
    for chunk in range(chunks):
        if chunk == 0:
            packed = kernel(
                functools.partial(pack_kernel, STEPS, in_ways[0]),
                pairs,
                pltpu.with_memory_space_constraint(x, pltpu.HBM),
                in_specs=[pl.BlockSpec(memory_space=pltpu.HBM)],
                scratch_shapes=[pltpu.VMEM((register, amp, register), F32), pltpu.SemaphoreType.DMA((STEPS,))],
            )
            near, other = kernel(part_kernel, halves, *along(packed, in_ways[0]))
            arrived.append([near, across(other)])
        else:
            own = x[:, chunk * amp : (chunk + 1) * amp, :]
            packed = kernel(functools.partial(pack_both_kernel, in_ways[chunk]), pairs, own, across(own))
            arrived.append(along(packed, in_ways[chunk]))

    gates = [swap(gate_blocks[0], k, sections, "segment") for k in range(sections)]
    low, high = kernel(
        functools.partial(combine_kernel, sections),
        [array(sections, 2 * register, 2 * register, dtype=BF16)] * 2,
        kraus_picks[0],
        block_targets,
        *gates,
        in_specs=[SMEM, SMEM] + [VMEM] * sections,
    )

    carried, held = [], []
    for chunk, pieces in enumerate(arrived):
        last = chunk == chunks - 1
        both = 2 * register + EXTRA
        aside = array((lines - 1) * register + EXTRA, register)
        results = kernel(
            functools.partial(sections_kernel, sections, lines, (in_ways[chunk], out_ways[chunk]), len(pieces), last),
            [array(both, register), aside, aside] if last else pairs + [array(EXTRA, register)],
            *pieces,
            low,
            high,
            *carried,
            scratch_shapes=[pltpu.VMEM((amp, register, register), F32)],
        )
        if last:
            first, own, other = results
            first = shift(first, 1, lines, out_ways[chunk])
            tall = [array(both, register)] * (lines - 1)
            joined = kernel(join_kernel, tall, own, across(other))
            held += [shift(piece, k, lines, out_ways[chunk]) for k, piece in zip(later_turns(lines), joined)]
            tall = [array(register + EXTRA, register)] * 2
            near, other = kernel(part_last_kernel, tall, first)
            held += [near, across(other)]
        else:
            carried = [results[lines]]
            near, other = kernel(part_kernel, halves, *along(results[:lines], out_ways[chunk]))
            held += [near, across(other)]

    out, logs = kernel(
        functools.partial(unpack_kernel, lines, out_ways, chunks - 1, OUT_STEPS, float(amp_local * amp)),
        [array(register, middle, register), array(1, sections)],
        *held,
        out_specs=[pl.BlockSpec(memory_space=pltpu.HBM)] * 2,
        scratch_shapes=[
            pltpu.VMEM((register, middle, register), F32),
            pltpu.VMEM((1, sections), F32),
            pltpu.SemaphoreType.DMA((OUT_STEPS + 1,)),
        ],
    )
    return out.reshape(1, amp_local), logs


def noise_factors(kraus_rows):
    qubit_count = kraus_rows.shape[-1]
    register = 2**qubit_count
    positions = jnp.arange(register, dtype=jnp.int32)
    product = jnp.ones(kraus_rows.shape[:-1] + (register,), jnp.float32)
    for qubit_pos in range(qubit_count):
        bit_value = jnp.right_shift(positions, qubit_count - 1 - qubit_pos) & 1
        column = kraus_rows[..., qubit_pos : qubit_pos + 1]
        low_value = jnp.zeros(column.shape, jnp.float32)
        high_value = jnp.zeros(column.shape, jnp.float32)
        for option in range(4):
            picked = (column == option).astype(jnp.float32)
            low_value = low_value + picked * KEEP_FACTORS[option]
            high_value = high_value + picked * FLIP_FACTORS[option]
        product = product * jnp.where(bit_value == 1, high_value, low_value)
    return product


def apply_gate(amplitudes, matrix, factors, target):

    def on_low(values):
        mixed_rows = jnp.einsum("bhmk,ik->bhmi", values, matrix, precision=lax.Precision.HIGHEST)
        return mixed_rows * factors[:, None, None, :]

    def on_high(values):
        mixed_rows = jnp.einsum("bjmk,ij->bimk", values, matrix, precision=lax.Precision.HIGHEST)
        return mixed_rows * factors[:, :, None, None]

    return lax.cond(target == 0, on_low, on_high, amplitudes)


def square_sums(values):
    return (values, jnp.sum(values * values, axis=(1, 2, 3)))


def body_general(states, gate_blocks, kraus_picks, block_targets):
    traj_here = states.shape[0]
    amp_local = states.shape[1]
    register = gate_blocks.shape[-1]
    blocks = gate_blocks.shape[1]
    middle = amp_local // (register * register)
    total_amps = amp_local * lax.axis_size("amp")
    sections = lax.axis_size("segment")
    amplitudes = states.reshape(traj_here, register, middle, register)
    local_sums = [jnp.sum(amplitudes * amplitudes, axis=(1, 2, 3))]
    for section in range(sections):
        owned = jnp.where(lax.axis_index("segment") == section, gate_blocks, jnp.zeros_like(gate_blocks))
        section_gates = lax.psum(owned, "segment")[0]
        for block_pos in range(blocks):
            factors = noise_factors(kraus_picks[:, section, block_pos, :])
            amplitudes = apply_gate(
                amplitudes, section_gates[block_pos], factors, block_targets[section, block_pos]
            )
        amplitudes, local_sq = square_sums(
            lax.all_to_all(amplitudes, "amp", split_axis=1, concat_axis=1, tiled=True)
        )
        local_sums.append(local_sq)
    totals = lax.psum(jnp.stack(local_sums, axis=1), "amp")
    log_weights = jnp.log(totals[:, 1:] / totals[:, :-1])
    amplitudes = amplitudes / jnp.sqrt(totals[:, -1] / total_amps)[:, None, None, None]
    return (amplitudes.reshape(traj_here, amp_local), log_weights)


def solution(mesh):
    in_specs = (
        P("segment", "amp"),
        P("segment", None, None, None),
        P("segment", None, None, None),
        P(),
    )
    out_specs = (P("segment", "amp"), P("segment", None))
    amp, sections = mesh.shape["amp"], mesh.shape["segment"]

    def run(states, gate_blocks, kraus_picks, block_targets):
        register = gate_blocks.shape[-1]
        middle = states.shape[1] // amp // (register * register)
        power_of_two = amp > 2 and amp & (amp - 1) == 0 and sections & (sections - 1) == 0
        fits = middle > 0 and middle % amp == 0 and register % (8 * amp) == 0
        fast = power_of_two and fits and sections % 2 == 0 and sections < EXTRA and states.shape[0] == sections

        def body(*args):
            return (body_fast if fast else body_general)(*args)

        step = jax.shard_map(body, mesh=mesh, in_specs=in_specs, out_specs=out_specs, check_vma=False)
        return step(states, gate_blocks, kraus_picks, block_targets)

    return run
```

```python
import functools

import jax
import jax.numpy as jnp
from jax import lax
from jax.experimental import pallas as pl
from jax.experimental.pallas import tpu as pltpu
from jax.sharding import PartitionSpec as P


KEEP_FACTORS = (1.0, 0.9, 1.0, 0.97)
FLIP_FACTORS = (0.9, 1.0, 0.97, 1.0)
F32 = jnp.float32
BF16 = jnp.bfloat16
VMEM = pl.BlockSpec(memory_space=pltpu.VMEM)
SMEM = pl.BlockSpec(memory_space=pltpu.SMEM)
EXTRA = 8
OUT_STEPS = 8
IN_WAYS = (0, 0)
OUT_WAYS = (0, 1)
VMEM_LIMIT = 12 * 2**20


def device_at(me, step, near, lines, way):
    line = (me // 2) ^ step if way == 0 else (me // 2 + way * step) & (lines - 1)
    return 2 * line + ((me % 2) ^ near)


def split(value):
    high = value.astype(BF16)
    return high, (value - high.astype(F32)).astype(BF16)


def take_kernel(steps, lines, way, pairs_ref, *refs):
    me = lax.axis_index("amp")
    out_refs, sems = refs[:-1], refs[-1]
    copies = []
    for at, (step, out) in enumerate(zip(steps, out_refs)):
        pair = device_at(me, step, 0, lines, way) // 2
        copies.append(pltpu.make_async_copy(pairs_ref.at[:, pair], out, sems.at[at]))
        copies[-1].start()
    for copy in copies:
        copy.wait()


def pack_both_kernel(way, x_ref, side_ref, *out_refs):
    me = lax.axis_index("amp")
    register, middle, lanes = x_ref.shape
    for near, ref in enumerate((x_ref, side_ref)):
        rows = ref.reshape(register * middle, lanes)
        for far, out in enumerate(out_refs):
            out[near] = rows[pl.ds(device_at(me, far, 0, len(out_refs), way), register, stride=middle), :]


def part_kernel(*refs):
    lines = len(refs) - 2
    for far in range(lines):
        refs[lines][far] = refs[far][0]
        refs[lines + 1][far] = refs[far][1]


def part_first_kernel(*refs):
    lines = len(refs) - 2
    south = lax.axis_index("amp") % 2 == 0
    for far in range(lines):
        values = refs[far][:, 0, :], refs[far][:, 1, :]
        refs[lines][far] = jnp.where(south, values[0], values[1])
        refs[lines + 1][far] = jnp.where(south, values[1], values[0])


def part_last_kernel(piece_ref, near_ref, other_ref):
    register = near_ref.shape[1]
    sums = piece_ref[2 * register :, :]
    for near, out in enumerate((near_ref, other_ref)):
        out[:register, :] = piece_ref[near * register : (near + 1) * register, :]
        out[register:, :] = sums


def join_kernel(own_ref, other_ref, *out_refs):
    register = own_ref.shape[1]
    last = len(out_refs) * register
    sums = own_ref[last:, :] + other_ref[last:, :]
    for far, out in enumerate(out_refs):
        for near, ref in enumerate((own_ref, other_ref)):
            out[near * register : (near + 1) * register, :] = ref[far * register : (far + 1) * register, :]
        out[2 * register :, :] = sums


def pick_of(pick, factors):
    value = jnp.float32(factors[-1])
    for option in range(len(factors) - 1):
        value = jnp.where(pick == option, factors[option], value)
    return value


def noise_rows(picks_ref, section, block, register):
    rows = lax.broadcasted_iota(jnp.int32, (register, register), 0)
    product = jnp.ones((register, register), F32)
    qubits = picks_ref.shape[-1]
    for q in range(qubits):
        pick = picks_ref[section, block, q]
        bit = jnp.right_shift(rows, qubits - 1 - q) & 1
        product = product * jnp.where(bit == 1, pick_of(pick, FLIP_FACTORS), pick_of(pick, KEEP_FACTORS))
    return product


def combine_kernel(sections, picks_ref, targets_ref, *refs):
    gate_refs, (low_ref, high_ref) = refs[:sections], refs[sections:]
    seg = lax.axis_index("segment")
    blocks, register = gate_refs[0].shape[0], gate_refs[0].shape[-1]
    rows = lax.broadcasted_iota(jnp.int32, (register, register), 0)
    columns = lax.broadcasted_iota(jnp.int32, (register, register), 1)
    eye = (rows == columns).astype(F32)
    zero = jnp.zeros((register, register), BF16)
    for k in range(sections):
        section = seg ^ k
        low, high = eye, eye
        for block in range(blocks):
            on_low = targets_ref[section, block] == 0
            moved = gate_refs[k][block] * noise_rows(picks_ref, section, block, register)
            if block > 0:
                before = jnp.where(on_low, low, high)
                moved = jnp.dot(moved, before, precision=lax.Precision.HIGHEST, preferred_element_type=F32)
            low, high = jnp.where(on_low, moved, low), jnp.where(on_low, high, moved)
        big, small = split(low.T)
        low_ref[section] = jnp.concatenate(
            [jnp.concatenate([big, small], axis=1), jnp.concatenate([big, zero], axis=1)], axis=0
        )
        big, small = split(high)
        high_ref[section] = jnp.concatenate(
            [jnp.concatenate([big, big], axis=1), jnp.concatenate([small, zero], axis=1)], axis=0
        )


def on_low(value, weights):
    lanes = value.shape[1]
    both = jnp.dot(jnp.concatenate(split(value), axis=1), weights, preferred_element_type=F32)
    return both[:, :lanes] + both[:, lanes:]


def on_high(value, weights):
    rows = value.shape[0] // 2
    wide = jnp.concatenate([value[:rows], value[rows:]], axis=1)
    both = jnp.dot(weights, jnp.concatenate(split(wide), axis=0), preferred_element_type=F32)
    both = both[:rows] + both[rows:]
    lanes = value.shape[1]
    return jnp.concatenate([both[:, :lanes], both[:, lanes:]], axis=0)


def piece_of(refs, far, near):
    return refs[near].at[far] if len(refs) == 2 else refs[far].at[near]


def later_turns(lines):
    return [turn for turn in range(lines) if turn != 1]


def sections_kernel(sections, lines, ways, pieces, last, *refs):
    amp = 2 * lines
    piece_refs, (low_ref, high_ref) = refs[:pieces], refs[pieces : pieces + 2]
    at = pieces + 2
    if last:
        sums_in, at = refs[at], at + 1
    out_refs, x = refs[at:-1], refs[-1]
    me = lax.axis_index("amp")
    register, lanes = piece_refs[0].shape[-2:]
    rest = register // amp

    def squares(total, value):
        return total + jnp.sum(value * value, axis=0, keepdims=True)

    total = jnp.zeros((1, lanes), F32)
    for far in range(lines):
        for near in range(2):
            value = piece_of(piece_refs, far, near)[...]
            total = squares(total, value)
            x[device_at(me, far, near, lines, -ways[0])] = value
    sums = [total]
    for section in range(sections):
        low, high = low_ref[section], high_ref[section]
        total = jnp.zeros((1, lanes), F32)
        for pair in range(lines):
            parts = (2 * pair, 2 * pair + 1)
            if section % 2 == 0:
                value = jnp.concatenate([x[part] for part in parts], axis=0)
            else:
                spans = [x[:, part * rest : (part + 1) * rest, :].reshape(register, lanes) for part in parts]
                value = jnp.concatenate(spans, axis=0)
            value = on_high(on_low(value, low), high)
            total = squares(total, value)
            for half, part in enumerate(parts):
                piece = value[half * register : (half + 1) * register]
                if section % 2 == 0:
                    x[part] = piece
                else:
                    x[:, part * rest : (part + 1) * rest, :] = piece.reshape(amp, rest, lanes)
        sums.append(total)
    rows = jnp.concatenate(sums + [jnp.zeros((EXTRA - len(sums), lanes), F32)], axis=0)
    if not last:
        for far in range(lines):
            for near in range(2):
                out_refs[far][near] = x[device_at(me, far, near, lines, ways[1])]
        out_refs[lines][...] = rows
        return
    rows = rows + sums_in[...]
    first = out_refs[0]
    for near in range(2):
        first[near * register : (near + 1) * register, :] = x[device_at(me, 1, near, lines, ways[1])]
        for at, far in enumerate(later_turns(lines)):
            out_refs[1 + near][at * register : (at + 1) * register, :] = x[device_at(me, far, near, lines, ways[1])]
        out_refs[1 + near][(lines - 1) * register :, :] = rows
    first[2 * register :, :] = rows


def unpack_kernel(lines, ways, early, steps, total_amps, *refs):
    held, refs = refs[: 2 * early], refs[2 * early :]
    joined, first_refs, (x_ref, logs_ref, out, logs_held, sems) = refs[: lines - 1], refs[lines - 1 : lines + 1], refs[lines + 1 :]
    me = lax.axis_index("amp")
    register, middle, lanes = out.shape
    sections = logs_ref.shape[1]
    totals = first_refs[0][register:, :] + first_refs[1][register:, :]
    for ref in joined:
        totals = totals + ref[2 * register :, :]
    totals = jnp.sum(totals, axis=1, keepdims=True)
    scale = 1.0 / jnp.sqrt(totals[sections : sections + 1] / total_amps)
    flat = out.reshape(register * middle, lanes)
    step = register // steps
    copies = []
    for at in range(steps):
        low, high = at * step, (at + 1) * step
        for chunk in range(early + 1):
            for far in range(lines):
                for near in range(2):
                    if chunk < early:
                        value = held[2 * chunk + near][far, low:high, :]
                    else:
                        if far == 1:
                            value = first_refs[near][low:high, :]
                        else:
                            at_turn = later_turns(lines).index(far)
                            value = joined[at_turn][near * register + low : near * register + high, :]
                    m = chunk * 2 * lines + device_at(me, far, near, lines, -ways[chunk])
                    flat[pl.ds(low * middle + m, step, stride=middle), :] = value * scale
        span = pl.ds(low, step)
        copies.append(pltpu.make_async_copy(out.at[span], x_ref.at[span], sems.at[at]))
        copies[-1].start()
    logs = jnp.log(totals[1 : sections + 1] / totals[:sections])
    rows = lax.broadcasted_iota(jnp.int32, (sections, sections), 0)
    columns = lax.broadcasted_iota(jnp.int32, (sections, sections), 1)
    logs_held[...] = jnp.sum(jnp.where(rows == columns, logs, 0.0), axis=0, keepdims=True)
    copies.append(pltpu.make_async_copy(logs_held, logs_ref, sems.at[steps]))
    copies[-1].start()
    for copy in copies:
        copy.wait()


def swap(piece, k, size, axis):
    if k == 0:
        return piece
    return lax.ppermute(piece, axis, [(i, i ^ k) for i in range(size)])


def shift(piece, step, lines, way):
    if step == 0:
        return piece
    pairs = [(me, device_at(me, step, 0, lines, way)) for me in range(2 * lines)]
    return lax.ppermute(piece, "amp", pairs)


def body_fast(states, gate_blocks, kraus_picks, block_targets):
    amp_local = states.shape[1]
    register = gate_blocks.shape[-1]
    amp, sections = lax.axis_size("amp"), lax.axis_size("segment")
    middle = amp_local // (register * register)
    chunks, lines = middle // amp, amp // 2
    in_ways, out_ways = [IN_WAYS[chunk > 0] for chunk in range(chunks)], [OUT_WAYS[chunk == chunks - 1] for chunk in range(chunks)]
    params = pltpu.CompilerParams(vmem_limit_bytes=VMEM_LIMIT)

    def array(*shape, dtype=F32):
        return jax.ShapeDtypeStruct(shape, dtype)

    def kernel(body, out_shape, *operands, **options):
        specs = dict(in_specs=[VMEM] * len(operands), out_specs=[VMEM] * len(out_shape))
        return pl.pallas_call(body, out_shape=out_shape, compiler_params=params, **{**specs, **options})(*operands)

    def along(pieces, way):
        return [shift(piece, step, lines, way) for step, piece in enumerate(pieces)]

    def across(piece):
        return swap(piece, 1, amp, "amp")

    pairs, halves = [array(2, register, register)] * lines, [array(lines, register, register)] * 2
    x = states.reshape(register, middle, register)
    arrived = []
    for chunk in range(chunks):
        if chunk == 0:
            by_pairs = pltpu.with_memory_space_constraint(states.reshape(register, middle // 2, 2, register), pltpu.HBM)
            packed = {}
            for steps in ([lines - 1], list(range(lines - 1))):
                taken = kernel(
                    functools.partial(take_kernel, steps, lines, in_ways[0]),
                    [array(register, 2, register)] * len(steps),
                    by_pairs,
                    in_specs=[pl.BlockSpec(memory_space=pltpu.HBM)],
                    scratch_shapes=[pltpu.SemaphoreType.DMA((len(steps),))],
                )
                packed.update(zip(steps, taken))
            pieces = along([packed[step] for step in range(lines)], in_ways[0])
            near, other = kernel(part_first_kernel, halves, *pieces)
            arrived.append([near, across(other)])
        else:
            own = x[:, chunk * amp : (chunk + 1) * amp, :]
            packed = kernel(functools.partial(pack_both_kernel, in_ways[chunk]), pairs, own, across(own))
            arrived.append(along(packed, in_ways[chunk]))

    gates = [swap(gate_blocks[0], k, sections, "segment") for k in range(sections)]
    low, high = kernel(
        functools.partial(combine_kernel, sections),
        [array(sections, 2 * register, 2 * register, dtype=BF16)] * 2,
        kraus_picks[0],
        block_targets,
        *gates,
        in_specs=[SMEM, SMEM] + [VMEM] * sections,
    )

    carried, held = [], []
    for chunk, pieces in enumerate(arrived):
        last = chunk == chunks - 1
        both = 2 * register + EXTRA
        aside = array((lines - 1) * register + EXTRA, register)
        results = kernel(
            functools.partial(sections_kernel, sections, lines, (in_ways[chunk], out_ways[chunk]), len(pieces), last),
            [array(both, register), aside, aside] if last else pairs + [array(EXTRA, register)],
            *pieces,
            low,
            high,
            *carried,
            scratch_shapes=[pltpu.VMEM((amp, register, register), F32)],
        )
        if last:
            first, own, other = results
            first = shift(first, 1, lines, out_ways[chunk])
            tall = [array(both, register)] * (lines - 1)
            joined = kernel(join_kernel, tall, own, across(other))
            held += [shift(piece, k, lines, out_ways[chunk]) for k, piece in zip(later_turns(lines), joined)]
            tall = [array(register + EXTRA, register)] * 2
            near, other = kernel(part_last_kernel, tall, first)
            held += [near, across(other)]
        else:
            carried = [results[lines]]
            near, other = kernel(part_kernel, halves, *along(results[:lines], out_ways[chunk]))
            held += [near, across(other)]

    out, logs = kernel(
        functools.partial(unpack_kernel, lines, out_ways, chunks - 1, OUT_STEPS, float(amp_local * amp)),
        [array(register, middle, register), array(1, sections)],
        *held,
        out_specs=[pl.BlockSpec(memory_space=pltpu.HBM)] * 2,
        scratch_shapes=[
            pltpu.VMEM((register, middle, register), F32),
            pltpu.VMEM((1, sections), F32),
            pltpu.SemaphoreType.DMA((OUT_STEPS + 1,)),
        ],
    )
    return out.reshape(1, amp_local), logs


def noise_factors(kraus_rows):
    qubit_count = kraus_rows.shape[-1]
    register = 2**qubit_count
    positions = jnp.arange(register, dtype=jnp.int32)
    product = jnp.ones(kraus_rows.shape[:-1] + (register,), jnp.float32)
    for qubit_pos in range(qubit_count):
        bit_value = jnp.right_shift(positions, qubit_count - 1 - qubit_pos) & 1
        column = kraus_rows[..., qubit_pos : qubit_pos + 1]
        low_value = jnp.zeros(column.shape, jnp.float32)
        high_value = jnp.zeros(column.shape, jnp.float32)
        for option in range(4):
            picked = (column == option).astype(jnp.float32)
            low_value = low_value + picked * KEEP_FACTORS[option]
            high_value = high_value + picked * FLIP_FACTORS[option]
        product = product * jnp.where(bit_value == 1, high_value, low_value)
    return product


def apply_gate(amplitudes, matrix, factors, target):

    def on_low(values):
        mixed_rows = jnp.einsum("bhmk,ik->bhmi", values, matrix, precision=lax.Precision.HIGHEST)
        return mixed_rows * factors[:, None, None, :]

    def on_high(values):
        mixed_rows = jnp.einsum("bjmk,ij->bimk", values, matrix, precision=lax.Precision.HIGHEST)
        return mixed_rows * factors[:, :, None, None]

    return lax.cond(target == 0, on_low, on_high, amplitudes)


def square_sums(values):
    return (values, jnp.sum(values * values, axis=(1, 2, 3)))


def body_general(states, gate_blocks, kraus_picks, block_targets):
    traj_here = states.shape[0]
    amp_local = states.shape[1]
    register = gate_blocks.shape[-1]
    blocks = gate_blocks.shape[1]
    middle = amp_local // (register * register)
    total_amps = amp_local * lax.axis_size("amp")
    sections = lax.axis_size("segment")
    amplitudes = states.reshape(traj_here, register, middle, register)
    local_sums = [jnp.sum(amplitudes * amplitudes, axis=(1, 2, 3))]
    for section in range(sections):
        owned = jnp.where(lax.axis_index("segment") == section, gate_blocks, jnp.zeros_like(gate_blocks))
        section_gates = lax.psum(owned, "segment")[0]
        for block_pos in range(blocks):
            factors = noise_factors(kraus_picks[:, section, block_pos, :])
            amplitudes = apply_gate(
                amplitudes, section_gates[block_pos], factors, block_targets[section, block_pos]
            )
        amplitudes, local_sq = square_sums(
            lax.all_to_all(amplitudes, "amp", split_axis=1, concat_axis=1, tiled=True)
        )
        local_sums.append(local_sq)
    totals = lax.psum(jnp.stack(local_sums, axis=1), "amp")
    log_weights = jnp.log(totals[:, 1:] / totals[:, :-1])
    amplitudes = amplitudes / jnp.sqrt(totals[:, -1] / total_amps)[:, None, None, None]
    return (amplitudes.reshape(traj_here, amp_local), log_weights)


def solution(mesh):
    in_specs = (
        P("segment", "amp"),
        P("segment", None, None, None),
        P("segment", None, None, None),
        P(),
    )
    out_specs = (P("segment", "amp"), P("segment", None))
    amp, sections = mesh.shape["amp"], mesh.shape["segment"]

    def run(states, gate_blocks, kraus_picks, block_targets):
        register = gate_blocks.shape[-1]
        middle = states.shape[1] // amp // (register * register)
        power_of_two = amp > 2 and amp & (amp - 1) == 0 and sections & (sections - 1) == 0
        fits = middle > 0 and middle % amp == 0 and register % (8 * amp) == 0
        fast = power_of_two and fits and sections % 2 == 0 and sections < EXTRA and states.shape[0] == sections

        def body(*args):
            return (body_fast if fast else body_general)(*args)

        step = jax.shard_map(body, mesh=mesh, in_specs=in_specs, out_specs=out_specs, check_vma=False)
        return step(states, gate_blocks, kraus_picks, block_targets)

    return run
```

```python
import functools

import jax
import jax.numpy as jnp
from jax import lax
from jax.experimental import pallas as pl
from jax.experimental.pallas import tpu as pltpu
from jax.sharding import PartitionSpec as P


KEEP_FACTORS = (1.0, 0.9, 1.0, 0.97)
FLIP_FACTORS = (0.9, 1.0, 0.97, 1.0)
F32 = jnp.float32
BF16 = jnp.bfloat16
VMEM = pl.BlockSpec(memory_space=pltpu.VMEM)
SMEM = pl.BlockSpec(memory_space=pltpu.SMEM)
EXTRA = 8
OUT_STEPS = 8
IN_WAYS = (0, 0)
OUT_WAYS = (0, 1)
VMEM_LIMIT = 12 * 2**20


def device_at(me, step, near, lines, way):
    line = (me // 2) ^ step if way == 0 else (me // 2 + way * step) & (lines - 1)
    return 2 * line + ((me % 2) ^ near)


def split(value):
    high = value.astype(BF16)
    return high, (value - high.astype(F32)).astype(BF16)


def take_kernel(steps, lines, way, pairs_ref, *refs):
    me = lax.axis_index("amp")
    out_refs, sems = refs[:-1], refs[-1]
    copies = []
    for at, (step, out) in enumerate(zip(steps, out_refs)):
        pair = device_at(me, step, 0, lines, way) // 2
        copies.append(pltpu.make_async_copy(pairs_ref.at[:, pair], out, sems.at[at]))
        copies[-1].start()
    for copy in copies:
        copy.wait()


def pack_both_kernel(way, x_ref, side_ref, *out_refs):
    me = lax.axis_index("amp")
    register, middle, lanes = x_ref.shape
    for near, ref in enumerate((x_ref, side_ref)):
        rows = ref.reshape(register * middle, lanes)
        for far, out in enumerate(out_refs):
            out[near] = rows[pl.ds(device_at(me, far, 0, len(out_refs), way), register, stride=middle), :]


def part_kernel(*refs):
    lines = len(refs) - 2
    for far in range(lines):
        refs[lines][far] = refs[far][0]
        refs[lines + 1][far] = refs[far][1]


def part_first_kernel(*refs):
    lines = len(refs) - 2
    south = lax.axis_index("amp") % 2 == 0
    for far in range(lines):
        values = refs[far][:, 0, :], refs[far][:, 1, :]
        refs[lines][far] = jnp.where(south, values[0], values[1])
        refs[lines + 1][far] = jnp.where(south, values[1], values[0])


def part_last_kernel(piece_ref, near_ref, other_ref, sums_ref):
    register = near_ref.shape[0]
    near_ref[...] = piece_ref[:register, :]
    other_ref[...] = piece_ref[register : 2 * register, :]
    sums_ref[...] = piece_ref[2 * register : 2 * register + 1, :]


def join_kernel(own_ref, other_ref, *out_refs):
    register = own_ref.shape[1]
    for far, out in enumerate(out_refs):
        for near, ref in enumerate((own_ref, other_ref)):
            out[near * register : (near + 1) * register, :] = ref[far * register : (far + 1) * register, :]


def in_one_row(rows_of_sums):
    totals = jnp.broadcast_to(jnp.sum(rows_of_sums, axis=1, keepdims=True), rows_of_sums.shape)
    rows, columns = (lax.broadcasted_iota(jnp.int32, rows_of_sums.shape, axis) for axis in range(2))
    return jnp.sum(jnp.where(rows == columns, totals, 0.0), axis=0, keepdims=True)


def line_kernel(*refs):
    total = refs[0][...]
    for ref in refs[1:-1]:
        total = total + ref[...]
    refs[-1][...] = total


def total_kernel(total_amps, *refs):
    parts, (logs_ref, scale_ref) = refs[:-2], refs[-2:]
    totals = parts[0][...]
    for part in parts[1:]:
        totals = totals + part[...]
    sections = logs_ref.shape[1]
    logs_ref[...] = jnp.log(totals[:, 1 : sections + 1] / totals[:, :sections])
    scale = 1.0 / jnp.sqrt(totals[:, sections : sections + 1] / total_amps)
    scale_ref[...] = jnp.broadcast_to(scale, scale_ref.shape)


def pick_of(pick, factors):
    value = jnp.float32(factors[-1])
    for option in range(len(factors) - 1):
        value = jnp.where(pick == option, factors[option], value)
    return value


def noise_rows(picks_ref, section, block, register):
    rows = lax.broadcasted_iota(jnp.int32, (register, register), 0)
    product = jnp.ones((register, register), F32)
    qubits = picks_ref.shape[-1]
    for q in range(qubits):
        pick = picks_ref[section, block, q]
        bit = jnp.right_shift(rows, qubits - 1 - q) & 1
        product = product * jnp.where(bit == 1, pick_of(pick, FLIP_FACTORS), pick_of(pick, KEEP_FACTORS))
    return product


def combine_kernel(sections, picks_ref, targets_ref, *refs):
    gate_refs, (low_ref, high_ref) = refs[:sections], refs[sections:]
    seg = lax.axis_index("segment")
    blocks, register = gate_refs[0].shape[0], gate_refs[0].shape[-1]
    rows = lax.broadcasted_iota(jnp.int32, (register, register), 0)
    columns = lax.broadcasted_iota(jnp.int32, (register, register), 1)
    eye = (rows == columns).astype(F32)
    zero = jnp.zeros((register, register), BF16)
    for k in range(sections):
        section = seg ^ k
        low, high = eye, eye
        for block in range(blocks):
            on_low = targets_ref[section, block] == 0
            moved = gate_refs[k][block] * noise_rows(picks_ref, section, block, register)
            if block > 0:
                before = jnp.where(on_low, low, high)
                moved = jnp.dot(moved, before, precision=lax.Precision.HIGHEST, preferred_element_type=F32)
            low, high = jnp.where(on_low, moved, low), jnp.where(on_low, high, moved)
        big, small = split(low.T)
        low_ref[section] = jnp.concatenate(
            [jnp.concatenate([big, small], axis=1), jnp.concatenate([big, zero], axis=1)], axis=0
        )
        big, small = split(high)
        high_ref[section] = jnp.concatenate(
            [jnp.concatenate([big, big], axis=1), jnp.concatenate([small, zero], axis=1)], axis=0
        )


def on_low(value, weights):
    lanes = value.shape[1]
    both = jnp.dot(jnp.concatenate(split(value), axis=1), weights, preferred_element_type=F32)
    return both[:, :lanes] + both[:, lanes:]


def on_high(value, weights):
    rows = value.shape[0] // 2
    wide = jnp.concatenate([value[:rows], value[rows:]], axis=1)
    both = jnp.dot(weights, jnp.concatenate(split(wide), axis=0), preferred_element_type=F32)
    both = both[:rows] + both[rows:]
    lanes = value.shape[1]
    return jnp.concatenate([both[:, :lanes], both[:, lanes:]], axis=0)


def piece_of(refs, far, near):
    return refs[near].at[far] if len(refs) == 2 else refs[far].at[near]


def later_turns(lines):
    return [turn for turn in range(lines) if turn != 1]


def sections_kernel(sections, lines, ways, pieces, last, *refs):
    amp = 2 * lines
    piece_refs, (low_ref, high_ref) = refs[:pieces], refs[pieces : pieces + 2]
    at = pieces + 2
    if last:
        sums_in, at = refs[at], at + 1
    out_refs, x = refs[at:-1], refs[-1]
    me = lax.axis_index("amp")
    register, lanes = piece_refs[0].shape[-2:]
    rest = register // amp

    def squares(total, value):
        return total + jnp.sum(value * value, axis=0, keepdims=True)

    total = jnp.zeros((1, lanes), F32)
    for far in range(lines):
        for near in range(2):
            value = piece_of(piece_refs, far, near)[...]
            total = squares(total, value)
            x[device_at(me, far, near, lines, -ways[0])] = value
    sums = [total]
    for section in range(sections):
        low, high = low_ref[section], high_ref[section]
        total = jnp.zeros((1, lanes), F32)
        for pair in range(lines):
            parts = (2 * pair, 2 * pair + 1)
            if section % 2 == 0:
                value = jnp.concatenate([x[part] for part in parts], axis=0)
            else:
                spans = [x[:, part * rest : (part + 1) * rest, :].reshape(register, lanes) for part in parts]
                value = jnp.concatenate(spans, axis=0)
            value = on_high(on_low(value, low), high)
            total = squares(total, value)
            for half, part in enumerate(parts):
                piece = value[half * register : (half + 1) * register]
                if section % 2 == 0:
                    x[part] = piece
                else:
                    x[:, part * rest : (part + 1) * rest, :] = piece.reshape(amp, rest, lanes)
        sums.append(total)
    rows = jnp.concatenate(sums + [jnp.zeros((EXTRA - len(sums), lanes), F32)], axis=0)
    if not last:
        for far in range(lines):
            for near in range(2):
                out_refs[far][near] = x[device_at(me, far, near, lines, ways[1])]
        out_refs[lines][...] = rows
        return
    rows = rows + sums_in[...]
    first, sums = out_refs[0], in_one_row(rows)
    first[2 * register :, :] = jnp.broadcast_to(sums, rows.shape)
    out_refs[3][...] = sums
    for near in range(2):
        first[near * register : (near + 1) * register, :] = x[device_at(me, 1, near, lines, ways[1])]
        for at, far in enumerate(later_turns(lines)):
            out_refs[1 + near][at * register : (at + 1) * register, :] = x[device_at(me, far, near, lines, ways[1])]


def unpack_kernel(lines, ways, early, scale_ref, logs_in, *refs):
    held, refs = refs[: 2 * early], refs[2 * early :]
    joined, first_refs, (x_ref, logs_ref, out, sems) = refs[: lines - 1], refs[lines - 1 : lines + 1], refs[lines + 1 :]
    me = lax.axis_index("amp")
    register, middle, lanes = out.shape
    scale = scale_ref[0:1, :]
    flat = out.reshape(register * middle, lanes)
    steps = sems.shape[0] - 1
    size = register // steps
    copies = [pltpu.make_async_copy(logs_in, logs_ref, sems.at[steps])]
    copies[0].start()
    for at in range(steps):
        low, high = at * size, (at + 1) * size
        for chunk in range(early + 1):
            for far in range(lines):
                for near in range(2):
                    if chunk < early:
                        value = held[2 * chunk + near][far, low:high, :]
                    elif far == 1:
                        value = first_refs[near][low:high, :]
                    else:
                        at_turn = later_turns(lines).index(far)
                        value = joined[at_turn][near * register + low : near * register + high, :]
                    m = chunk * 2 * lines + device_at(me, far, near, lines, -ways[chunk])
                    flat[pl.ds(low * middle + m, size, stride=middle), :] = value * scale
        span = pl.ds(low, size)
        copies.append(pltpu.make_async_copy(out.at[span], x_ref.at[span], sems.at[at]))
        copies[-1].start()
    for copy in copies:
        copy.wait()


def swap(piece, k, size, axis):
    if k == 0:
        return piece
    return lax.ppermute(piece, axis, [(i, i ^ k) for i in range(size)])


def shift(piece, step, lines, way):
    if step == 0:
        return piece
    pairs = [(me, device_at(me, step, 0, lines, way)) for me in range(2 * lines)]
    return lax.ppermute(piece, "amp", pairs)


def body_fast(states, gate_blocks, kraus_picks, block_targets):
    amp_local = states.shape[1]
    register = gate_blocks.shape[-1]
    amp, sections = lax.axis_size("amp"), lax.axis_size("segment")
    middle = amp_local // (register * register)
    chunks, lines = middle // amp, amp // 2
    in_ways, out_ways = [IN_WAYS[chunk > 0] for chunk in range(chunks)], [OUT_WAYS[chunk == chunks - 1] for chunk in range(chunks)]
    params = pltpu.CompilerParams(vmem_limit_bytes=VMEM_LIMIT)

    def array(*shape, dtype=F32):
        return jax.ShapeDtypeStruct(shape, dtype)

    def kernel(body, out_shape, *operands, **options):
        specs = dict(in_specs=[VMEM] * len(operands), out_specs=[VMEM] * len(out_shape))
        return pl.pallas_call(body, out_shape=out_shape, compiler_params=params, **{**specs, **options})(*operands)

    def along(pieces, way):
        return [shift(piece, step, lines, way) for step, piece in enumerate(pieces)]

    def across(piece):
        return swap(piece, 1, amp, "amp")

    pairs, halves = [array(2, register, register)] * lines, [array(lines, register, register)] * 2
    x = states.reshape(register, middle, register)
    arrived = []
    for chunk in range(chunks):
        if chunk == 0:
            by_pairs = pltpu.with_memory_space_constraint(states.reshape(register, middle // 2, 2, register), pltpu.HBM)
            packed = {}
            for steps in ([lines - 1], list(range(lines - 1))):
                taken = kernel(
                    functools.partial(take_kernel, steps, lines, in_ways[0]),
                    [array(register, 2, register)] * len(steps),
                    by_pairs,
                    in_specs=[pl.BlockSpec(memory_space=pltpu.HBM)],
                    scratch_shapes=[pltpu.SemaphoreType.DMA((len(steps),))],
                )
                packed.update(zip(steps, taken))
            pieces = along([packed[step] for step in range(lines)], in_ways[0])
            near, other = kernel(part_first_kernel, halves, *pieces)
            arrived.append([near, across(other)])
        else:
            own = x[:, chunk * amp : (chunk + 1) * amp, :]
            packed = kernel(functools.partial(pack_both_kernel, in_ways[chunk]), pairs, own, across(own))
            arrived.append(along(packed, in_ways[chunk]))

    gates = [swap(gate_blocks[0], k, sections, "segment") for k in range(sections)]
    low, high = kernel(
        functools.partial(combine_kernel, sections),
        [array(sections, 2 * register, 2 * register, dtype=BF16)] * 2,
        kraus_picks[0],
        block_targets,
        *gates,
        in_specs=[SMEM, SMEM] + [VMEM] * sections,
    )

    carried, held = [], []
    for chunk, pieces in enumerate(arrived):
        last = chunk == chunks - 1
        both = 2 * register
        aside = array((lines - 1) * register, register)
        results = kernel(
            functools.partial(sections_kernel, sections, lines, (in_ways[chunk], out_ways[chunk]), len(pieces), last),
            [array(both + EXTRA, register), aside, aside, array(1, register)] if last else pairs + [array(EXTRA, register)],
            *pieces,
            low,
            high,
            *carried,
            scratch_shapes=[pltpu.VMEM((amp, register, register), F32)],
        )
        if last:
            first, own, other, sums = results
            first = shift(first, 1, lines, out_ways[chunk])
            tall = [array(both, register)] * (lines - 1)
            joined = kernel(join_kernel, tall, own, across(other))
            late = [shift(piece, k, lines, out_ways[chunk]) for k, piece in zip(later_turns(lines), joined)]
            parts = [shift(sums, k, lines, 1) for k in later_turns(lines)]
            square, row = array(register, register), array(1, register)
            near, other, sums = kernel(part_last_kernel, [square, square, row], first)
            (sums,) = kernel(line_kernel, [row], sums, *parts)
            parts = [sums, across(sums)]
            late += [near, across(other)]
        else:
            carried = [results[lines]]
            near, other = kernel(part_kernel, halves, *along(results[:lines], out_ways[chunk]))
            held += [near, across(other)]

    logs, scale = kernel(
        functools.partial(total_kernel, float(amp_local * amp)), [array(1, sections), array(8, register)], *parts
    )
    out, logs = kernel(
        functools.partial(unpack_kernel, lines, out_ways, chunks - 1),
        [array(register, middle, register), array(1, sections)],
        scale,
        logs,
        *held,
        *late,
        out_specs=[pl.BlockSpec(memory_space=pltpu.HBM)] * 2,
        scratch_shapes=[pltpu.VMEM((register, middle, register), F32), pltpu.SemaphoreType.DMA((OUT_STEPS + 1,))],
    )
    return out.reshape(1, amp_local), logs


def noise_factors(kraus_rows):
    qubit_count = kraus_rows.shape[-1]
    register = 2**qubit_count
    positions = jnp.arange(register, dtype=jnp.int32)
    product = jnp.ones(kraus_rows.shape[:-1] + (register,), jnp.float32)
    for qubit_pos in range(qubit_count):
        bit_value = jnp.right_shift(positions, qubit_count - 1 - qubit_pos) & 1
        column = kraus_rows[..., qubit_pos : qubit_pos + 1]
        low_value = jnp.zeros(column.shape, jnp.float32)
        high_value = jnp.zeros(column.shape, jnp.float32)
        for option in range(4):
            picked = (column == option).astype(jnp.float32)
            low_value = low_value + picked * KEEP_FACTORS[option]
            high_value = high_value + picked * FLIP_FACTORS[option]
        product = product * jnp.where(bit_value == 1, high_value, low_value)
    return product


def apply_gate(amplitudes, matrix, factors, target):

    def on_low(values):
        mixed_rows = jnp.einsum("bhmk,ik->bhmi", values, matrix, precision=lax.Precision.HIGHEST)
        return mixed_rows * factors[:, None, None, :]

    def on_high(values):
        mixed_rows = jnp.einsum("bjmk,ij->bimk", values, matrix, precision=lax.Precision.HIGHEST)
        return mixed_rows * factors[:, :, None, None]

    return lax.cond(target == 0, on_low, on_high, amplitudes)


def square_sums(values):
    return (values, jnp.sum(values * values, axis=(1, 2, 3)))


def body_general(states, gate_blocks, kraus_picks, block_targets):
    traj_here = states.shape[0]
    amp_local = states.shape[1]
    register = gate_blocks.shape[-1]
    blocks = gate_blocks.shape[1]
    middle = amp_local // (register * register)
    total_amps = amp_local * lax.axis_size("amp")
    sections = lax.axis_size("segment")
    amplitudes = states.reshape(traj_here, register, middle, register)
    local_sums = [jnp.sum(amplitudes * amplitudes, axis=(1, 2, 3))]
    for section in range(sections):
        owned = jnp.where(lax.axis_index("segment") == section, gate_blocks, jnp.zeros_like(gate_blocks))
        section_gates = lax.psum(owned, "segment")[0]
        for block_pos in range(blocks):
            factors = noise_factors(kraus_picks[:, section, block_pos, :])
            amplitudes = apply_gate(
                amplitudes, section_gates[block_pos], factors, block_targets[section, block_pos]
            )
        amplitudes, local_sq = square_sums(
            lax.all_to_all(amplitudes, "amp", split_axis=1, concat_axis=1, tiled=True)
        )
        local_sums.append(local_sq)
    totals = lax.psum(jnp.stack(local_sums, axis=1), "amp")
    log_weights = jnp.log(totals[:, 1:] / totals[:, :-1])
    amplitudes = amplitudes / jnp.sqrt(totals[:, -1] / total_amps)[:, None, None, None]
    return (amplitudes.reshape(traj_here, amp_local), log_weights)


def solution(mesh):
    in_specs = (
        P("segment", "amp"),
        P("segment", None, None, None),
        P("segment", None, None, None),
        P(),
    )
    out_specs = (P("segment", "amp"), P("segment", None))
    amp, sections = mesh.shape["amp"], mesh.shape["segment"]

    def run(states, gate_blocks, kraus_picks, block_targets):
        register = gate_blocks.shape[-1]
        middle = states.shape[1] // amp // (register * register)
        power_of_two = amp > 2 and amp & (amp - 1) == 0 and sections & (sections - 1) == 0
        fits = middle > amp and middle % amp == 0 and register % (8 * amp) == 0
        fast = power_of_two and fits and sections % 2 == 0 and sections < EXTRA and states.shape[0] == sections

        def body(*args):
            return (body_fast if fast else body_general)(*args)

        step = jax.shard_map(body, mesh=mesh, in_specs=in_specs, out_specs=out_specs, check_vma=False)
        return step(states, gate_blocks, kraus_picks, block_targets)

    return run
```
